32 devices in a mesh: dp: 16 (over z, y, x), tensor: 2 (over core).
Axes of the slice: x: 2, y: 2, z: 4, core: 2. Of those that a mesh axis runs over, the one named last changes fastest.
Arguments:
- tokens: bfloat16 [18432, 768], P(('dp', 'tensor')), may hold values from -6 to 6
- ln1_gain: bfloat16 [768], replicated, may hold values from 0.5 to 1.5
- ln1_bias: bfloat16 [768], replicated, may hold values from -1.75 to 1.75
- qkv_weight: bfloat16 [3, 768, 768], P(None, None, 'tensor'), may hold values from -0.3125 to 0.3125
- qv_bias: bfloat16 [2, 768], P(None, 'tensor'), may hold values from -1.75 to 1.75
- out_weight: bfloat16 [768, 768], P('tensor'), may hold values from -0.625 to 0.625
- out_bias: bfloat16 [768], replicated, may hold values from -1.75 to 1.75
- ln2_gain: bfloat16 [768], replicated, may hold values from 0.5 to 1.5
- ln2_bias: bfloat16 [768], replicated, may hold values from -1.75 to 1.75
- fc_weight: bfloat16 [768, 3072], P(None, 'tensor'), may hold values from -0.21875 to 0.21875
- fc_bias: bfloat16 [3072], P('tensor'), may hold values from -3 to 3
- proj_weight: bfloat16 [3072, 768], P('tensor'), may hold values from -0.15625 to 0.15625
- proj_bias: bfloat16 [768], replicated, may hold values from -1.75 to 1.75
- cotangent: bfloat16 [18432, 768], P(('dp', 'tensor')), may hold values from -6 to 6
Outputs:
- block_output: bfloat16 [18432, 768], P(('dp', 'tensor'))
- input_grad: bfloat16 [18432, 768], P(('dp', 'tensor'))
- grad_ln1_gain: float32 [768], replicated
- grad_ln1_bias: float32 [768], replicated
- grad_qkv_weight: float32 [3, 768, 768], P(None, None, 'tensor')
- grad_qv_bias: float32 [2, 768], P(None, 'tensor')
- grad_out_weight: float32 [768, 768], P('tensor')
- grad_out_bias: float32 [768], replicated
- grad_ln2_gain: float32 [768], replicated
- grad_ln2_bias: float32 [768], replicated
- grad_fc_weight: float32 [768, 3072], P(None, 'tensor')
- grad_fc_bias: float32 [3072], P('tensor')
- grad_proj_weight: float32 [3072, 768], P('tensor')
- grad_proj_bias: float32 [768], replicated
The draws below stay inside these ranges and needn't reach their ends.
All inputs are finite; a program needn't handle non-finite values.
Results may differ from the reference program's by a relative error of at most 0.014.
The reference program's roundings to bfloat16 on the way count: a program that leaves them out, or rounds other values in their place, can miss the bound.
Values may be sent and summed in bfloat16 or wider, within the bound.
A program may use at most 192 MiB of HBM per device.

```python
import jax
import jax.numpy as jnp
from jax import lax

D = 768
HEADS = 12
HD = 64
FF = 3072
PROMPT = 896
CONT = 128
NCONT = 2
GROUP = 1152
TOKENS = 18432
N_DP = 16


def steps_of(own_key, shape, split, smallest, top_value):
    factor_of, own = 1.0, jax.random.fold_in(own_key, 6)
    for position, shards_of in split:
        heights = jnp.exp(jax.random.uniform(jax.random.fold_in(own, position), (shards_of,), jnp.float32, smallest / len(split), top_value / len(split)))
        factor_of = factor_of * jnp.repeat(heights, shape[position] // shards_of).reshape([-1 if axis == position else 1 for axis in range(len(shape))])
    return factor_of


def normal_values(stream_key, dims, width, bound, split=(), kind=jnp.bfloat16):
    drawn = jax.random.normal(stream_key, dims, jnp.float32) * width
    if len(split) > 0:
        drawn = steps_of(stream_key, dims, split, -0.22, 0.18) * drawn
    return jnp.clip(drawn, min=-bound, max=bound).astype(kind)


def setup_inputs(seed: int = 0) -> dict:
    arg_keys = jax.random.split(jax.random.key(seed), 15)
    tokens = normal_values(arg_keys[0], (TOKENS, D), 1.0, 6.0, ((0, 32),))
    ln1_gain = jnp.clip(1.0 + 0.1 * jax.random.normal(arg_keys[1], (D,), jnp.float32), 0.5, 1.5).astype(jnp.bfloat16)
    ln1_bias = normal_values(arg_keys[2], (D,), 0.3, 1.75)
    qkv_weight = normal_values(arg_keys[3], (3, D, D), (D // 2) ** -0.5, 0.3125, ((2, 2),))
    qv_bias = normal_values(arg_keys[4], (2, D), 0.3, 1.75, ((1, 2),))
    out_weight = normal_values(arg_keys[5], (D, D), (D // 8) ** -0.5, 0.625, ((0, 2),))
    out_bias = normal_values(arg_keys[6], (D,), 0.3, 1.75)
    ln2_gain = jnp.clip(1.0 + 0.1 * jax.random.normal(arg_keys[7], (D,), jnp.float32), 0.5, 1.5).astype(jnp.bfloat16)
    ln2_bias = normal_values(arg_keys[8], (D,), 0.3, 1.75)
    fc_weight = normal_values(arg_keys[9], (D, FF), D ** -0.5, 0.21875, ((1, 2),))
    fc_bias = normal_values(arg_keys[10], (FF,), 0.5, 3.0, ((0, 2),))
    proj_weight = normal_values(arg_keys[11], (FF, D), (FF // 2) ** -0.5, 0.15625, ((0, 2),))
    proj_bias = normal_values(arg_keys[12], (D,), 0.3, 1.75)
    cotangent = normal_values(arg_keys[13], (TOKENS, D), 1.0, 6.0, ((0, 32),))
    return dict(tokens=tokens, ln1_gain=ln1_gain, ln1_bias=ln1_bias, qkv_weight=qkv_weight, qv_bias=qv_bias, out_weight=out_weight, out_bias=out_bias, ln2_gain=ln2_gain, ln2_bias=ln2_bias, fc_weight=fc_weight, fc_bias=fc_bias, proj_weight=proj_weight, proj_bias=proj_bias, cotangent=cotangent)


PRECISE = lax.Precision.HIGHEST
EPSILON = 1e-05
MASKED = -1e+30

@jax.custom_vjp
def low(v):
    return lax.optimization_barrier(v.astype(jnp.bfloat16)).astype(jnp.float32)

@jax.custom_vjp
def low_back(v):
    return v

def low_keep(v):
    return (low(v), None)

def low_pass(kept, grad):
    return (grad,)

def back_keep(v):
    return (v, None)

def back_low(kept, grad):
    return (low(grad),)
low.defvjp(low_keep, low_pass)
low_back.defvjp(back_keep, back_low)

def layer_norm(values, gain_vec, shift_vec):
    mean_row = lax.optimization_barrier(jnp.mean(values, axis=-1, keepdims=True))
    centred = values - mean_row
    return centred * lax.rsqrt(lax.optimization_barrier(jnp.mean(centred * centred, axis=-1, keepdims=True)) + EPSILON) * gain_vec + shift_vec

def causal_mask(length):
    row_pos = lax.broadcasted_iota(jnp.int32, (length, length), 0)
    col_pos = lax.broadcasted_iota(jnp.int32, (length, length), 1)
    return col_pos <= row_pos

def attend(queries, keys_all, values):
    score_scale = HD ** (-0.5)
    q_head = queries[:PROMPT]
    k_head = keys_all[:PROMPT]
    v_head = values[:PROMPT]
    q_tail = queries[PROMPT:].reshape(NCONT, CONT, HEADS, HD)
    k_tail = keys_all[PROMPT:].reshape(NCONT, CONT, HEADS, HD)
    v_tail = values[PROMPT:].reshape(NCONT, CONT, HEADS, HD)
    scores = jnp.einsum('qha,kha->hqk', q_head, k_head, precision=PRECISE) * score_scale
    scores = jnp.where(causal_mask(PROMPT), low_back(scores), MASKED)
    attn_probs = low(jax.nn.softmax(scores, axis=-1))
    out_head = jnp.einsum('hqk,kha->qha', attn_probs, v_head, precision=PRECISE)
    far_scores = jnp.einsum('ncha,kha->nhck', q_tail, k_head, precision=PRECISE) * score_scale
    near_scores = jnp.einsum('ncha,ndha->nhcd', q_tail, k_tail, precision=PRECISE) * score_scale
    all_scores = low_back(jnp.concatenate([far_scores, near_scores], axis=-1))
    allowed = jnp.concatenate([jnp.ones((CONT, PROMPT), dtype=bool), causal_mask(CONT)], axis=-1)
    all_scores = jnp.where(allowed, all_scores, MASKED)
    tail_probs = low(jax.nn.softmax(all_scores, axis=-1))
    out_tail = jnp.einsum('nhck,kha->ncha', tail_probs[..., :PROMPT], v_head, precision=PRECISE)
    out_tail = out_tail + jnp.einsum('nhcd,ndha->ncha', tail_probs[..., PROMPT:], v_tail, precision=PRECISE)
    return jnp.concatenate([out_head, out_tail.reshape(NCONT * CONT, HEADS, HD)], axis=0)

def layer(tokens, ln1_gain, ln1_bias, qkv_weight, qv_bias, out_weight, out_bias, ln2_gain, ln2_bias, fc_weight, fc_bias, proj_weight, proj_bias):
    normed = low(layer_norm(tokens, ln1_gain, ln1_bias))
    projected = jnp.einsum('gd,tdj->gtj', normed, qkv_weight, precision=PRECISE)
    bias_rows = jnp.stack([qv_bias[0], jnp.zeros_like(qv_bias[0]), qv_bias[1]])
    projected = low_back(low(projected + bias_rows))
    queries = projected[:, 0].reshape(GROUP, HEADS, HD)
    keys_all = projected[:, 1].reshape(GROUP, HEADS, HD)
    values = projected[:, 2].reshape(GROUP, HEADS, HD)
    mixed_heads = low_back(low(attend(queries, keys_all, values).reshape(GROUP, D)))
    attn_out = low_back(jnp.dot(mixed_heads, out_weight, precision=PRECISE) + out_bias)
    residual = tokens + attn_out
    normed2 = low(layer_norm(residual, ln2_gain, ln2_bias))
    pre_act = low_back(jnp.dot(normed2, fc_weight, precision=PRECISE) + fc_bias)
    activation = low(jax.nn.gelu(pre_act, approximate=True))
    branch = low_back(jnp.dot(activation, proj_weight, precision=PRECISE) + proj_bias)
    return residual + branch

def reference(tokens, ln1_gain, ln1_bias, qkv_weight, qv_bias, out_weight, out_bias, ln2_gain, ln2_bias, fc_weight, fc_bias, proj_weight, proj_bias, cotangent):
    params = tuple((p.astype(jnp.float32) for p in (ln1_gain, ln1_bias, qkv_weight, qv_bias, out_weight, out_bias, ln2_gain, ln2_bias, fc_weight, fc_bias, proj_weight, proj_bias)))
    group_tokens = tokens.astype(jnp.float32).reshape(N_DP, GROUP, D)
    group_cots = cotangent.astype(jnp.float32).reshape(N_DP, GROUP, D)

    def per_group(totals, pieces):
        block_in, block_cot = pieces
        output_now, pullback = jax.vjp(layer, block_in, *params)
        gradients = pullback(block_cot)
        totals = tuple((a + b for a, b in zip(totals, gradients[1:])))
        return (totals, (output_now.astype(jnp.bfloat16), gradients[0].astype(jnp.bfloat16)))
    zero_grads = tuple((jnp.zeros(p.shape, jnp.float32) for p in params))
    totals, (outputs, input_grads) = lax.scan(per_group, zero_grads, (group_tokens, group_cots))
    return (outputs.reshape(TOKENS, D), input_grads.reshape(TOKENS, D), totals[0], totals[1], totals[2], totals[3], totals[4], totals[5], totals[6], totals[7], totals[8], totals[9], totals[10], totals[11])
```

```python
import functools
import jax
import jax.numpy as jnp
from jax import lax
from jax.experimental import pallas as pl
from jax.experimental.pallas import tpu as pltpu

from jax.sharding import PartitionSpec as P

HD = 64
PROMPT = 896
CONT = 128
NCONT = 2


EPSILON = 1e-05
MASKED = -1e30


def norm_rows(values, gain_vec, shift_vec):
    mean_row = jnp.mean(values, axis=-1, keepdims=True)
    centred = values - mean_row
    inv_std = lax.rsqrt(jnp.mean(centred * centred, axis=-1, keepdims=True) + EPSILON)
    normal = centred * inv_std
    return (normal * gain_vec + shift_vec, normal, inv_std)


def norm_back(grad_out, normal, inv_std, gain_vec):
    scaled = grad_out * gain_vec
    inner = (
        scaled
        - jnp.mean(scaled, axis=-1, keepdims=True)
        - normal * jnp.mean(scaled * normal, axis=-1, keepdims=True)
    )
    return inner * inv_std


def split_group(values):
    head_part = values[:PROMPT]
    tail_part = values[PROMPT:].reshape(NCONT, CONT, values.shape[1], values.shape[2])
    return (head_part, tail_part)


def causal_mask(length):
    row_pos = lax.broadcasted_iota(jnp.int32, (length, length), 0)
    col_pos = lax.broadcasted_iota(jnp.int32, (length, length), 1)
    return col_pos <= row_pos


def prompt_scores(q_head, k_head):
    scores = jnp.einsum(
        "qha,kha->hqk", q_head, k_head, preferred_element_type=jnp.float32
    ) * HD ** (-0.5)
    return jnp.where(causal_mask(PROMPT), scores, MASKED)


def tail_scores(q_tail, k_head, k_tail):
    far_scores = jnp.einsum(
        "ncha,kha->nhck", q_tail, k_head, preferred_element_type=jnp.float32
    ) * HD ** (-0.5)
    near_scores = jnp.einsum(
        "ncha,ndha->nhcd", q_tail, k_tail, preferred_element_type=jnp.float32
    ) * HD ** (-0.5)
    return (far_scores, jnp.where(causal_mask(CONT), near_scores, MASKED))


def attend_forward(queries, keys_all, values):
    q_head, q_tail = split_group(queries)
    k_head, k_tail = split_group(keys_all)
    v_head, v_tail = split_group(values)
    scores = prompt_scores(q_head, k_head)
    top_head = jnp.max(scores, axis=-1, keepdims=True)
    expo_head = jnp.exp(scores - top_head)
    total_head = jnp.sum(expo_head, axis=-1, keepdims=True)
    prob_head = (expo_head / total_head).astype(jnp.bfloat16)
    lse_head = top_head + jnp.log(total_head)
    out_head = jnp.einsum("hqk,kha->qha", prob_head, v_head, preferred_element_type=jnp.float32)
    far_scores, near_scores = tail_scores(q_tail, k_head, k_tail)
    top_tail = jnp.maximum(
        jnp.max(far_scores, axis=-1, keepdims=True), jnp.max(near_scores, axis=-1, keepdims=True)
    )
    expo_far = jnp.exp(far_scores - top_tail)
    expo_near = jnp.exp(near_scores - top_tail)
    total_tail = jnp.sum(expo_far, axis=-1, keepdims=True) + jnp.sum(
        expo_near, axis=-1, keepdims=True
    )
    prob_far = (expo_far / total_tail).astype(jnp.bfloat16)
    prob_near = (expo_near / total_tail).astype(jnp.bfloat16)
    lse_tail = top_tail + jnp.log(total_tail)
    out_tail = jnp.einsum("nhck,kha->ncha", prob_far, v_head, preferred_element_type=jnp.float32)
    out_tail = out_tail + jnp.einsum(
        "nhcd,ndha->ncha", prob_near, v_tail, preferred_element_type=jnp.float32
    )
    heads_local = queries.shape[1]
    mixed = jnp.concatenate([out_head, out_tail.reshape(NCONT * CONT, heads_local, HD)], axis=0)
    return (mixed, lse_head, lse_tail)


def attend_back(queries, keys_all, values, grad_mixed, lse_head, lse_tail):
    q_head, q_tail = split_group(queries)
    k_head, k_tail = split_group(keys_all)
    v_head, v_tail = split_group(values)
    g_head, g_tail = split_group(grad_mixed)
    score_scale = HD ** (-0.5)
    prob_head = jnp.exp(prompt_scores(q_head, k_head) - lse_head)
    dprob_head = jnp.einsum("qha,kha->hqk", g_head, v_head, preferred_element_type=jnp.float32)
    row_dot = jnp.sum(prob_head * dprob_head, axis=-1, keepdims=True)
    dscore_head = (prob_head * (dprob_head - row_dot)).astype(jnp.bfloat16)
    dq_head = (
        jnp.einsum("hqk,kha->qha", dscore_head, k_head, preferred_element_type=jnp.float32)
        * score_scale
    )
    dk_head = (
        jnp.einsum("hqk,qha->kha", dscore_head, q_head, preferred_element_type=jnp.float32)
        * score_scale
    )
    dv_head = jnp.einsum(
        "hqk,qha->kha", prob_head.astype(jnp.bfloat16), g_head, preferred_element_type=jnp.float32
    )
    far_scores, near_scores = tail_scores(q_tail, k_head, k_tail)
    prob_far = jnp.exp(far_scores - lse_tail)
    prob_near = jnp.exp(near_scores - lse_tail)
    dprob_far = jnp.einsum("ncha,kha->nhck", g_tail, v_head, preferred_element_type=jnp.float32)
    dprob_near = jnp.einsum("ncha,ndha->nhcd", g_tail, v_tail, preferred_element_type=jnp.float32)
    tail_dot = jnp.sum(prob_far * dprob_far, axis=-1, keepdims=True) + jnp.sum(
        prob_near * dprob_near, axis=-1, keepdims=True
    )
    dscore_far = (prob_far * (dprob_far - tail_dot)).astype(jnp.bfloat16)
    dscore_near = (prob_near * (dprob_near - tail_dot)).astype(jnp.bfloat16)
    dq_tail = jnp.einsum("nhck,kha->ncha", dscore_far, k_head, preferred_element_type=jnp.float32)
    dq_tail = (
        dq_tail
        + jnp.einsum("nhcd,ndha->ncha", dscore_near, k_tail, preferred_element_type=jnp.float32)
    ) * score_scale
    dk_head = (
        dk_head
        + jnp.einsum("nhck,ncha->kha", dscore_far, q_tail, preferred_element_type=jnp.float32)
        * score_scale
    )
    dk_tail = (
        jnp.einsum("nhcd,ncha->ndha", dscore_near, q_tail, preferred_element_type=jnp.float32)
        * score_scale
    )
    dv_head = dv_head + jnp.einsum(
        "nhck,ncha->kha", prob_far.astype(jnp.bfloat16), g_tail, preferred_element_type=jnp.float32
    )
    dv_tail = jnp.einsum(
        "nhcd,ncha->ndha",
        prob_near.astype(jnp.bfloat16),
        g_tail,
        preferred_element_type=jnp.float32,
    )
    heads_local = queries.shape[1]
    tail_rows = NCONT * CONT
    grad_query = jnp.concatenate([dq_head, dq_tail.reshape(tail_rows, heads_local, HD)], axis=0)
    grad_key = jnp.concatenate([dk_head, dk_tail.reshape(tail_rows, heads_local, HD)], axis=0)
    grad_value = jnp.concatenate([dv_head, dv_tail.reshape(tail_rows, heads_local, HD)], axis=0)
    return (grad_query, grad_key, grad_value)


MESH = pl.DeviceIdType.MESH
ITEM = 1536
SMALL = 56
LN_ROWS = 24


class Sum:
    def __init__(self, part, res, rx1, rx2, rx3, ssem, rsem):
        self.part, self.res, self.rx1, self.rx2, self.rx3 = part, res, rx1, rx2, rx3
        self.ssem, self.rsem = ssem, rsem
        dp, t = lax.axis_index("dp"), lax.axis_index("tensor")
        x, y, z = lax.rem(dp, 2), lax.rem(lax.div(dp, 2), 2), lax.rem(lax.div(dp, 4), 4)
        self.t, self.z = t, z
        self.a = x * (1 - t) + y * t
        self.b = y * (1 - t) + x * t
        self.to_a = (dp + (1 + t) * (1 - 2 * self.a), t)
        self.to_b = (dp + (2 - t) * (1 - 2 * self.b), t)
        self.to_z = []
        self.zs = []
        for d in (1, 2, 3):
            zj = lax.rem(z + d, 4)
            self.zs.append(zj)
            self.to_z.append((dp + 4 * (zj - z), t))
        self.to_x = (dp + 1 - 2 * x, t)
        self.to_y = (dp + 2 - 4 * y, t)
        self.to_c = (dp, 1 - t)

    def barrier(self):
        bar = pltpu.get_barrier_semaphore()
        peers = [self.to_x, self.to_y, self.to_c] + self.to_z
        for peer in peers:
            pl.semaphore_signal(bar, inc=1, device_id=peer, device_id_type=MESH)
        pl.semaphore_wait(bar, len(peers))

    def rows(self, offset, count):
        return pl.ds(pl.multiple_of(offset, 32), count)

    def copy(self, src, dst, k, i, peer):
        return pltpu.make_async_remote_copy(
            src_ref=src, dst_ref=dst, send_sem=self.ssem.at[k, i], recv_sem=self.rsem.at[k, i],
            device_id=peer, device_id_type=MESH)

    def copies(self, stage, i):
        base = i * ITEM
        half = base + self.a * (ITEM // 2)
        quarter = half + self.b * (ITEM // 4)
        block = quarter + self.z * (ITEM // 16)
        if stage == 1:
            src = self.part.at[self.rows(base + (1 - self.a) * (ITEM // 2), ITEM // 2)]
            return [self.copy(src, self.rx1.at[self.rows(i * (ITEM // 2), ITEM // 2)], 0, i, self.to_a)]
        if stage == 2:
            src = self.part.at[self.rows(half + (1 - self.b) * (ITEM // 4), ITEM // 4)]
            return [self.copy(src, self.rx2.at[self.rows(i * (ITEM // 4), ITEM // 4)], 1, i, self.to_b)]
        if stage == 3:
            out = []
            for d in range(3):
                src = self.part.at[self.rows(quarter + self.zs[d] * (ITEM // 16), ITEM // 16)]
                dst = self.rx3.at[self.rows((i * 3 + d) * (ITEM // 16), ITEM // 16)]
                out.append(self.copy(src, dst, 2 + d, i, self.to_z[d]))
            return out
        if stage == 4:
            ref = self.res.at[self.rows(block, ITEM // 16)]
            return [self.copy(ref, ref, 5 + d, i, self.to_z[d]) for d in range(3)]
        if stage == 5:
            ref = self.res.at[self.rows(quarter, ITEM // 4)]
            return [self.copy(ref, ref, 8, i, self.to_b)]
        ref = self.res.at[self.rows(half, ITEM // 2)]
        return [self.copy(ref, ref, 9, i, self.to_a)]

    def start(self, stage, i):
        for c in self.copies(stage, i):
            c.start()

    def arrive(self, stage, i):
        for c in self.copies(stage, i):
            c.wait_recv()
        half = i * ITEM + self.a * (ITEM // 2)
        quarter = half + self.b * (ITEM // 4)
        block = quarter + self.z * (ITEM // 16)
        f32 = jnp.float32
        if stage == 1:
            own = self.rows(half, ITEM // 2)
            got = self.rx1[self.rows(i * (ITEM // 2), ITEM // 2), :]
            self.part[own, :] = (self.part[own, :].astype(f32) + got.astype(f32)).astype(jnp.bfloat16)
        elif stage == 2:
            own = self.rows(quarter, ITEM // 4)
            got = self.rx2[self.rows(i * (ITEM // 4), ITEM // 4), :]
            self.part[own, :] = (self.part[own, :].astype(f32) + got.astype(f32)).astype(jnp.bfloat16)
        elif stage == 3:
            own = self.rows(block, ITEM // 16)
            total = self.part[own, :].astype(f32)
            for d in range(3):
                total = total + self.rx3[self.rows((i * 3 + d) * (ITEM // 16), ITEM // 16), :].astype(f32)
            self.res[own, :] = total.astype(jnp.bfloat16)
        if stage < 6:
            self.start(stage + 1, i)

    def sent(self, i):
        for stage in range(1, 7):
            for c in self.copies(stage, i):
                c.wait_send()


def small_sum(comm, small, out, land_c, land_x, land_y, land_z, acc, ssem, rsem):
    def copy(src, dst, k, peer):
        return pltpu.make_async_remote_copy(
            src_ref=src, dst_ref=dst, send_sem=ssem.at[k], recv_sem=rsem.at[k],
            device_id=peer, device_id_type=MESH)

    c = copy(small.at[pl.ds(0, LN_ROWS)], land_c, 0, comm.to_c)
    c.start()
    yield
    c.wait_recv()
    acc[0] = small[...]
    acc[0, pl.ds(0, LN_ROWS), :] = small[pl.ds(0, LN_ROWS), :] + land_c[...]
    cx = copy(acc.at[0], land_x, 1, comm.to_x)
    cx.start()
    yield
    cx.wait_recv()
    acc[1] = acc[0] + land_x[...]
    cy = copy(acc.at[1], land_y, 2, comm.to_y)
    cy.start()
    yield
    cy.wait_recv()
    acc[2] = acc[1] + land_y[...]
    cz = []
    for d in range(3):
        cz.append(copy(acc.at[2], land_z.at[comm.z], 3 + d, comm.to_z[d]))
        cz[-1].start()
    yield
    land_z[comm.z] = acc[2]
    for d in range(3):
        cz[d].wait_recv()
    out[...] = (land_z[0] + land_z[1]) + (land_z[2] + land_z[3])
    for s in [c, cx, cy] + cz:
        s.wait_send()
    yield


def sum_kernel(n, part_in, small, res, small_out, part, rx1, rx2, rx3, ssem, rsem,
               land_c, land_x, land_y, land_z, acc, ss, sr, lsem):
    comm = Sum(part, res, rx1, rx2, rx3, ssem, rsem)
    load = pltpu.make_async_copy(part_in, part, lsem)
    load.start()
    comm.barrier()
    load.wait()
    sm = small_sum(comm, small, small_out, land_c, land_x, land_y, land_z, acc, ss, sr)
    next(sm)
    lax.fori_loop(0, n, lambda i, c: (comm.start(1, i), c)[1], 0)
    next(sm)

    def step(s, c):
        for stage in range(1, 7):
            i = s - (stage - 1)

            @pl.when((i >= 0) & (i < n))
            def _():
                comm.arrive(stage, i)
        return c

    lax.fori_loop(0, n + 5, step, 0)
    next(sm)
    next(sm)
    next(sm)
    lax.fori_loop(0, n, lambda i, c: (comm.sent(i), c)[1], 0)


def sum_call(part, small):
    n = part.shape[0] // ITEM
    f32, bf = jnp.float32, jnp.bfloat16
    return pl.pallas_call(
        functools.partial(sum_kernel, n),
        out_shape=(jax.ShapeDtypeStruct(part.shape, bf), jax.ShapeDtypeStruct(small.shape, f32)),
        in_specs=[pl.BlockSpec(memory_space=pl.ANY), pl.BlockSpec(memory_space=pltpu.VMEM)],
        out_specs=(pl.BlockSpec(memory_space=pltpu.VMEM), pl.BlockSpec(memory_space=pltpu.VMEM)),
        scratch_shapes=[
            pltpu.VMEM(part.shape, bf),
            pltpu.VMEM((n * ITEM // 2, 128), bf),
            pltpu.VMEM((n * ITEM // 4, 128), bf),
            pltpu.VMEM((n * 3 * ITEM // 16, 128), bf),
            pltpu.SemaphoreType.DMA((10, n)),
            pltpu.SemaphoreType.DMA((10, n)),
            pltpu.VMEM((LN_ROWS, 128), f32),
            pltpu.VMEM((SMALL, 128), f32),
            pltpu.VMEM((SMALL, 128), f32),
            pltpu.VMEM((4, SMALL, 128), f32),
            pltpu.VMEM((3, SMALL, 128), f32),
            pltpu.SemaphoreType.DMA((6,)),
            pltpu.SemaphoreType.DMA((6,)),
            pltpu.SemaphoreType.DMA,
        ],
        compiler_params=pltpu.CompilerParams(
            collective_id=0, has_side_effects=True, vmem_limit_bytes=56 * 2**20),
        name="grad_sum",
    )(part, small)


def swap(values):
    return lax.ppermute(values, "tensor", [(0, 1), (1, 0)])


def gather_pair(own):
    rows = own.shape[0]
    t = lax.axis_index("tensor")
    full = jnp.zeros((2 * rows,) + own.shape[1:], own.dtype)
    full = lax.dynamic_update_slice_in_dim(full, own, t * rows, 0)
    return lax.dynamic_update_slice_in_dim(full, swap(own), (1 - t) * rows, 0)


def scatter_pair(part):
    rows = part.shape[0] // 2
    t = lax.axis_index("tensor")
    away = lax.dynamic_slice_in_dim(part, (1 - t) * rows, rows, 0)
    return lax.dynamic_slice_in_dim(part, t * rows, rows, 0) + swap(away)


def blocks(values):
    lead, rows, cols = values.shape
    return values.reshape(lead, rows, cols // 128, 128).transpose(0, 2, 1, 3).reshape(-1, 128)


def unblock(stacked, lead, rows, cols):
    stacked = stacked.reshape(lead, cols // 128, rows, 128).astype(jnp.float32)
    return stacked.transpose(0, 2, 1, 3).reshape(lead, rows, cols)


def over_slice(values):
    count = lax.axis_size("dp")
    total = values
    for shift in range(16, count, 16):
        total = total + lax.ppermute(values, "dp", [(i, (i + shift) % count) for i in range(count)])
    return total


def on_device(
    tokens,
    ln1_gain,
    ln1_bias,
    qkv_weight,
    qv_bias,
    out_weight,
    out_bias,
    ln2_gain,
    ln2_bias,
    fc_weight,
    fc_bias,
    proj_weight,
    proj_bias,
    cotangent,
):
    own_rows = tokens.shape[0]
    group_rows = own_rows * lax.axis_size("tensor")
    local_width = qkv_weight.shape[2]
    heads_local = local_width // HD
    gain_one = ln1_gain.astype(jnp.float32)
    gain_two = ln2_gain.astype(jnp.float32)
    x_own = tokens.astype(jnp.float32)
    normed1, normal1, inv_std1 = norm_rows(x_own, gain_one, ln1_bias.astype(jnp.float32))
    ln1_full = gather_pair(normed1.astype(jnp.bfloat16))
    projected = jnp.einsum("gd,tdj->gtj", ln1_full, qkv_weight, preferred_element_type=jnp.float32)
    bias_float = qv_bias.astype(jnp.float32)
    bias_rows = jnp.stack([bias_float[0], jnp.zeros_like(bias_float[0]), bias_float[1]])
    projected = (projected + bias_rows).astype(jnp.bfloat16)
    queries = projected[:, 0].reshape(group_rows, heads_local, HD)
    keys_all = projected[:, 1].reshape(group_rows, heads_local, HD)
    values = projected[:, 2].reshape(group_rows, heads_local, HD)
    mixed, lse_head, lse_tail = attend_forward(queries, keys_all, values)
    mixed_low = mixed.reshape(group_rows, local_width).astype(jnp.bfloat16)
    part_rows = mixed_low
    attn_own = scatter_pair(jnp.dot(part_rows, out_weight, preferred_element_type=jnp.float32)) + out_bias.astype(jnp.float32)
    residual = x_own + attn_own
    normed2, normal2, inv_std2 = norm_rows(residual, gain_two, ln2_bias.astype(jnp.float32))
    ln2_full = gather_pair(normed2.astype(jnp.bfloat16))
    pre_act = jnp.dot(ln2_full, fc_weight, preferred_element_type=jnp.float32) + fc_bias.astype(
        jnp.float32
    )
    activation, gelu_pull = jax.vjp(lambda inner: jax.nn.gelu(inner, approximate=True), pre_act)
    act_low = activation.astype(jnp.bfloat16)
    part_rows = act_low
    mlp_own = scatter_pair(jnp.dot(part_rows, proj_weight, preferred_element_type=jnp.float32)) + proj_bias.astype(jnp.float32)
    block_output = (residual + mlp_own).astype(jnp.bfloat16)
    cot_full = gather_pair(cotangent)
    grad_proj_bias = jnp.sum(cot_full, axis=0, dtype=jnp.float32)
    grad_proj_weight = jnp.einsum(
        "gf,gd->fd", act_low, cot_full, preferred_element_type=jnp.float32
    )
    grad_act = jnp.einsum("gd,fd->gf", cot_full, proj_weight, preferred_element_type=jnp.float32)
    grad_pre = gelu_pull(grad_act)[0].astype(jnp.bfloat16)
    grad_fc_bias = jnp.sum(grad_pre, axis=0, dtype=jnp.float32)
    grad_fc_weight = jnp.einsum("gd,gf->df", ln2_full, grad_pre, preferred_element_type=jnp.float32)
    part_rows = grad_pre
    grad_norm2 = scatter_pair(jnp.einsum("gf,df->gd", part_rows, fc_weight, preferred_element_type=jnp.float32))
    grad_resid = cotangent.astype(jnp.float32) + norm_back(grad_norm2, normal2, inv_std2, gain_two)
    part_ln2_gain = jnp.sum(grad_norm2 * normal2, axis=0)
    part_ln2_bias = jnp.sum(grad_norm2, axis=0)
    attn_cot_full = gather_pair(grad_resid.astype(jnp.bfloat16))
    grad_out_bias = jnp.sum(attn_cot_full, axis=0, dtype=jnp.float32)
    grad_out_weight = jnp.einsum(
        "gj,gd->jd", mixed_low, attn_cot_full, preferred_element_type=jnp.float32
    )
    grad_mixed = jnp.einsum(
        "gd,jd->gj", attn_cot_full, out_weight, preferred_element_type=jnp.float32
    )
    grad_mixed = grad_mixed.astype(jnp.bfloat16).reshape(group_rows, heads_local, HD)
    grad_query, grad_key, grad_value = attend_back(
        queries, keys_all, values, grad_mixed, lse_head, lse_tail
    )
    grad_proj_all = (
        jnp.stack([grad_query, grad_key, grad_value], axis=1)
        .reshape(group_rows, 3, local_width)
        .astype(jnp.bfloat16)
    )
    grad_qkv_weight = jnp.einsum(
        "gd,gtj->tdj", ln1_full, grad_proj_all, preferred_element_type=jnp.float32
    )
    grad_qv_bias = jnp.sum(grad_proj_all[:, 0::2], axis=0, dtype=jnp.float32)
    part_rows = grad_proj_all
    grad_norm1 = scatter_pair(jnp.einsum("gtj,tdj->gd", part_rows, qkv_weight, preferred_element_type=jnp.float32))
    input_grad = (grad_resid + norm_back(grad_norm1, normal1, inv_std1, gain_one)).astype(
        jnp.bfloat16
    )
    part_ln1_gain = jnp.sum(grad_norm1 * normal1, axis=0)
    part_ln1_bias = jnp.sum(grad_norm1, axis=0)
    width = tokens.shape[1]
    units = fc_weight.shape[1]
    low = jnp.bfloat16
    part = jnp.concatenate(
        [
            blocks(grad_proj_weight.astype(low).reshape(units // 256, 256, width)),
            blocks(grad_fc_weight.astype(low)[None]),
            blocks(grad_out_weight.astype(low)[None]),
            blocks(grad_qkv_weight.astype(low)),
        ],
        axis=0,
    )
    small = jnp.concatenate(
        [
            part_ln1_gain,
            part_ln1_bias,
            part_ln2_gain,
            part_ln2_bias,
            grad_qv_bias.reshape(-1),
            grad_out_bias,
            grad_fc_bias,
            grad_proj_bias,
            jnp.zeros((SMALL * 128 - 6912,), jnp.float32),
        ]
    ).reshape(SMALL, 128)
    total, small = sum_call(part, small)
    cuts = [units * width // 128]
    cuts.append(cuts[-1] + units * width // 128)
    cuts.append(cuts[-1] + local_width * width // 128)
    grad_proj_weight = unblock(total[: cuts[0]], units // 256, 256, width).reshape(units, width)
    grad_fc_weight = unblock(total[cuts[0] : cuts[1]], 1, width, units)[0]
    grad_out_weight = unblock(total[cuts[1] : cuts[2]], 1, local_width, width)[0]
    grad_qkv_weight = unblock(total[cuts[2] :], 3, width, local_width)
    small = over_slice(small)
    if lax.axis_size("dp") > 16:
        grad_proj_weight = over_slice(grad_proj_weight)
        grad_fc_weight = over_slice(grad_fc_weight)
        grad_out_weight = over_slice(grad_out_weight)
        grad_qkv_weight = over_slice(grad_qkv_weight)
    flat = small.reshape(-1)
    grad_ln1_gain, grad_ln1_bias = flat[:768], flat[768:1536]
    grad_ln2_gain, grad_ln2_bias = flat[1536:2304], flat[2304:3072]
    grad_qv_bias = flat[3072:3840].reshape(2, local_width)
    grad_out_bias, grad_fc_bias, grad_proj_bias = flat[3840:4608], flat[4608:6144], flat[6144:6912]
    return (
        block_output,
        input_grad,
        grad_ln1_gain,
        grad_ln1_bias,
        grad_qkv_weight,
        grad_qv_bias,
        grad_out_weight,
        grad_out_bias,
        grad_ln2_gain,
        grad_ln2_bias,
        grad_fc_weight,
        grad_fc_bias,
        grad_proj_weight,
        grad_proj_bias,
    )


def solution(mesh):
    return jax.shard_map(
        on_device,
        mesh=mesh,
        in_specs=(
            P(("dp", "tensor"), None),
            P(),
            P(),
            P(None, None, "tensor"),
            P(None, "tensor"),
            P("tensor", None),
            P(),
            P(),
            P(),
            P(None, "tensor"),
            P("tensor"),
            P("tensor", None),
            P(),
            P(("dp", "tensor"), None),
        ),
        out_specs=(
            P(("dp", "tensor"), None),
            P(("dp", "tensor"), None),
            P(),
            P(),
            P(None, None, "tensor"),
            P(None, "tensor"),
            P("tensor", None),
            P(),
            P(),
            P(),
            P(None, "tensor"),
            P("tensor"),
            P("tensor", None),
            P(),
        ),
        check_vma=False,
    )
```

```python
import functools
import jax
import jax.numpy as jnp
from jax import lax
from jax.experimental import pallas as pl
from jax.experimental.pallas import tpu as pltpu

from jax.sharding import PartitionSpec as P

HD = 64
PROMPT = 896
CONT = 128
NCONT = 2


EPSILON = 1e-05
MASKED = -1e30


def norm_rows(values, gain_vec, shift_vec):
    mean_row = jnp.mean(values, axis=-1, keepdims=True)
    centred = values - mean_row
    inv_std = lax.rsqrt(jnp.mean(centred * centred, axis=-1, keepdims=True) + EPSILON)
    normal = centred * inv_std
    return (normal * gain_vec + shift_vec, normal, inv_std)


def norm_back(grad_out, normal, inv_std, gain_vec):
    scaled = grad_out * gain_vec
    inner = (
        scaled
        - jnp.mean(scaled, axis=-1, keepdims=True)
        - normal * jnp.mean(scaled * normal, axis=-1, keepdims=True)
    )
    return inner * inv_std


MESH = pl.DeviceIdType.MESH
ITEM = 1536
SMALL = 56
LN_ROWS = 24


class Sum:
    def __init__(self, part, res, rx1, rx2, rx3, ssem, rsem):
        self.part, self.res, self.rx1, self.rx2, self.rx3 = part, res, rx1, rx2, rx3
        self.ssem, self.rsem = ssem, rsem
        dp, t = lax.axis_index("dp"), lax.axis_index("tensor")
        x, y, z = lax.rem(dp, 2), lax.rem(lax.div(dp, 2), 2), lax.rem(lax.div(dp, 4), 4)
        self.t, self.z = t, z
        self.a = x * (1 - t) + y * t
        self.b = y * (1 - t) + x * t
        self.to_a = (dp + (1 + t) * (1 - 2 * self.a), t)
        self.to_b = (dp + (2 - t) * (1 - 2 * self.b), t)
        self.to_z = []
        self.zs = []
        for d in (1, 2, 3):
            zj = lax.rem(z + d, 4)
            self.zs.append(zj)
            self.to_z.append((dp + 4 * (zj - z), t))
        self.to_x = (dp + 1 - 2 * x, t)
        self.to_y = (dp + 2 - 4 * y, t)
        self.to_c = (dp, 1 - t)

    def barrier(self):
        bar = pltpu.get_barrier_semaphore()
        peers = [self.to_x, self.to_y, self.to_c] + self.to_z
        for peer in peers:
            pl.semaphore_signal(bar, inc=1, device_id=peer, device_id_type=MESH)
        pl.semaphore_wait(bar, len(peers))

    def rows(self, offset, count):
        return pl.ds(pl.multiple_of(offset, 32), count)

    def copy(self, src, dst, k, i, peer):
        return pltpu.make_async_remote_copy(
            src_ref=src, dst_ref=dst, send_sem=self.ssem.at[k, i], recv_sem=self.rsem.at[k, i],
            device_id=peer, device_id_type=MESH)

    def copies(self, stage, i):
        base = i * ITEM
        half = base + self.a * (ITEM // 2)
        quarter = half + self.b * (ITEM // 4)
        block = quarter + self.z * (ITEM // 16)
        if stage == 1:
            src = self.part.at[self.rows(base + (1 - self.a) * (ITEM // 2), ITEM // 2)]
            return [self.copy(src, self.rx1.at[self.rows(i * (ITEM // 2), ITEM // 2)], 0, i, self.to_a)]
        if stage == 2:
            src = self.part.at[self.rows(half + (1 - self.b) * (ITEM // 4), ITEM // 4)]
            return [self.copy(src, self.rx2.at[self.rows(i * (ITEM // 4), ITEM // 4)], 1, i, self.to_b)]
        if stage == 3:
            out = []
            for d in range(3):
                src = self.part.at[self.rows(quarter + self.zs[d] * (ITEM // 16), ITEM // 16)]
                dst = self.rx3.at[self.rows((i * 3 + d) * (ITEM // 16), ITEM // 16)]
                out.append(self.copy(src, dst, 2 + d, i, self.to_z[d]))
            return out
        if stage == 4:
            ref = self.res.at[self.rows(block, ITEM // 16)]
            return [self.copy(ref, ref, 5 + d, i, self.to_z[d]) for d in range(3)]
        if stage == 5:
            ref = self.res.at[self.rows(quarter, ITEM // 4)]
            return [self.copy(ref, ref, 8, i, self.to_b)]
        ref = self.res.at[self.rows(half, ITEM // 2)]
        return [self.copy(ref, ref, 9, i, self.to_a)]

    def start(self, stage, i):
        for c in self.copies(stage, i):
            c.start()

    def arrive(self, stage, i):
        for c in self.copies(stage, i):
            c.wait_recv()
        half = i * ITEM + self.a * (ITEM // 2)
        quarter = half + self.b * (ITEM // 4)
        block = quarter + self.z * (ITEM // 16)
        f32 = jnp.float32
        if stage == 1:
            own = self.rows(half, ITEM // 2)
            got = self.rx1[self.rows(i * (ITEM // 2), ITEM // 2), :]
            self.part[own, :] = (self.part[own, :].astype(f32) + got.astype(f32)).astype(jnp.bfloat16)
        elif stage == 2:
            own = self.rows(quarter, ITEM // 4)
            got = self.rx2[self.rows(i * (ITEM // 4), ITEM // 4), :]
            self.part[own, :] = (self.part[own, :].astype(f32) + got.astype(f32)).astype(jnp.bfloat16)
        elif stage == 3:
            own = self.rows(block, ITEM // 16)
            total = self.part[own, :].astype(f32)
            for d in range(3):
                total = total + self.rx3[self.rows((i * 3 + d) * (ITEM // 16), ITEM // 16), :].astype(f32)
            self.res[own, :] = total.astype(jnp.bfloat16)
        if stage < 6:
            self.start(stage + 1, i)

    def sent(self, i):
        for stage in range(1, 7):
            for c in self.copies(stage, i):
                c.wait_send()


def small_sum(comm, small, out, land_c, land_x, land_y, land_z, acc, ssem, rsem):
    def copy(src, dst, k, peer):
        return pltpu.make_async_remote_copy(
            src_ref=src, dst_ref=dst, send_sem=ssem.at[k], recv_sem=rsem.at[k],
            device_id=peer, device_id_type=MESH)

    c = copy(small.at[pl.ds(0, LN_ROWS)], land_c, 0, comm.to_c)
    c.start()
    yield
    c.wait_recv()
    acc[0] = small[...]
    acc[0, pl.ds(0, LN_ROWS), :] = small[pl.ds(0, LN_ROWS), :] + land_c[...]
    cx = copy(acc.at[0], land_x, 1, comm.to_x)
    cx.start()
    yield
    cx.wait_recv()
    acc[1] = acc[0] + land_x[...]
    cy = copy(acc.at[1], land_y, 2, comm.to_y)
    cy.start()
    yield
    cy.wait_recv()
    acc[2] = acc[1] + land_y[...]
    cz = []
    for d in range(3):
        cz.append(copy(acc.at[2], land_z.at[comm.z], 3 + d, comm.to_z[d]))
        cz[-1].start()
    yield
    land_z[comm.z] = acc[2]
    for d in range(3):
        cz[d].wait_recv()
    out[...] = (land_z[0] + land_z[1]) + (land_z[2] + land_z[3])
    for s in [c, cx, cy] + cz:
        s.wait_send()
    yield


def sum_kernel(n, *refs):
    (part_p, part_f, part_a, small, res, small_out, part, rx1, rx2, rx3, ssem, rsem,
     land_c, land_x, land_y, land_z, acc, ss, sr, lsem) = refs
    comm = Sum(part, res, rx1, rx2, rx3, ssem, rsem)
    third = n // 3 * ITEM
    loads = [
        pltpu.make_async_copy(ref, part.at[pl.ds(k * third, third)], lsem.at[k])
        for k, ref in enumerate((part_p, part_f, part_a))
    ]
    for load in loads:
        load.start()
    comm.barrier()
    for load in loads:
        load.wait()
    sm = small_sum(comm, small, small_out, land_c, land_x, land_y, land_z, acc, ss, sr)
    next(sm)
    lax.fori_loop(0, n, lambda i, c: (comm.start(1, i), c)[1], 0)
    next(sm)

    def step(s, c):
        for stage in range(1, 7):
            i = s - (stage - 1)

            @pl.when((i >= 0) & (i < n))
            def _():
                comm.arrive(stage, i)
        return c

    lax.fori_loop(0, n + 5, step, 0)
    next(sm)
    next(sm)
    next(sm)
    lax.fori_loop(0, n, lambda i, c: (comm.sent(i), c)[1], 0)


def sum_call(parts, small):
    shape = (sum(part.shape[0] for part in parts), 128)
    n = shape[0] // ITEM
    f32, bf = jnp.float32, jnp.bfloat16
    return pl.pallas_call(
        functools.partial(sum_kernel, n),
        out_shape=(jax.ShapeDtypeStruct(shape, bf), jax.ShapeDtypeStruct(small.shape, f32)),
        in_specs=[pl.BlockSpec(memory_space=pl.ANY)] * 3 + [pl.BlockSpec(memory_space=pltpu.VMEM)],
        out_specs=(pl.BlockSpec(memory_space=pltpu.VMEM), pl.BlockSpec(memory_space=pltpu.VMEM)),
        scratch_shapes=[
            pltpu.VMEM(shape, bf),
            pltpu.VMEM((n * ITEM // 2, 128), bf),
            pltpu.VMEM((n * ITEM // 4, 128), bf),
            pltpu.VMEM((n * 3 * ITEM // 16, 128), bf),
            pltpu.SemaphoreType.DMA((10, n)),
            pltpu.SemaphoreType.DMA((10, n)),
            pltpu.VMEM((LN_ROWS, 128), f32),
            pltpu.VMEM((SMALL, 128), f32),
            pltpu.VMEM((SMALL, 128), f32),
            pltpu.VMEM((4, SMALL, 128), f32),
            pltpu.VMEM((3, SMALL, 128), f32),
            pltpu.SemaphoreType.DMA((6,)),
            pltpu.SemaphoreType.DMA((6,)),
            pltpu.SemaphoreType.DMA((3,)),
        ],
        compiler_params=pltpu.CompilerParams(
            collective_id=0, has_side_effects=True, vmem_limit_bytes=56 * 2**20),
        name="grad_sum",
    )(*parts, small)


def swap(values):
    return lax.ppermute(values, "tensor", [(0, 1), (1, 0)])


def gather_pair(own):
    rows = own.shape[0]
    t = lax.axis_index("tensor")
    full = jnp.zeros((2 * rows,) + own.shape[1:], own.dtype)
    full = lax.dynamic_update_slice_in_dim(full, own, t * rows, 0)
    return lax.dynamic_update_slice_in_dim(full, swap(own), (1 - t) * rows, 0)


def scatter_pair(part):
    rows = part.shape[0] // 2
    t = lax.axis_index("tensor")
    away = lax.dynamic_slice_in_dim(part, (1 - t) * rows, rows, 0)
    return lax.dynamic_slice_in_dim(part, t * rows, rows, 0) + swap(away)


def dot(lhs, rhs, lhs_dim, rhs_dim):
    return lax.dot_general(
        lhs, rhs, (((lhs_dim,), (rhs_dim,)), ((), ())), preferred_element_type=jnp.float32)


BLOCK = 128
PROMPT_BLOCKS = PROMPT // BLOCK
GROUP = PROMPT + NCONT * CONT


def head_lanes(which):
    lane = lax.broadcasted_iota(jnp.int32, (1, 128), 1)
    return (lane >= which * HD) & (lane < (which + 1) * HD)


def own_mask():
    row_pos = lax.broadcasted_iota(jnp.int32, (BLOCK, BLOCK), 0)
    col_pos = lax.broadcasted_iota(jnp.int32, (BLOCK, BLOCK), 1)
    return col_pos <= row_pos


def key_ranges(block):
    start = block * BLOCK
    return min(start, PROMPT), start


def attend_kernel(q_ref, k_ref, v_ref, o_ref, lse_ref):
    scale = HD ** (-0.5)
    mask = own_mask()
    for block in range(GROUP // BLOCK):
        far, start = key_ranges(block)
        rows = slice(start, start + BLOCK)
        outs, lses = [], []
        for which in range(2):
            lanes = head_lanes(which)
            q = jnp.where(lanes, q_ref[0, rows, :], 0)
            near = jnp.where(mask, dot(q, k_ref[0, rows, :], 1, 1) * scale, MASKED)
            top = jnp.max(near, axis=-1, keepdims=True)
            if far:
                away = dot(q, k_ref[0, 0:far, :], 1, 1) * scale
                top = jnp.maximum(top, jnp.max(away, axis=-1, keepdims=True))
            near = jnp.exp(near - top)
            total = jnp.sum(near, axis=-1, keepdims=True)
            if far:
                away = jnp.exp(away - top)
                total = total + jnp.sum(away, axis=-1, keepdims=True)
            share = 1.0 / total
            out = dot((near * share).astype(jnp.bfloat16), v_ref[0, rows, :], 1, 0)
            if far:
                out = out + dot((away * share).astype(jnp.bfloat16), v_ref[0, 0:far, :], 1, 0)
            outs.append(out)
            lses.append(top + jnp.log(total))
        first = head_lanes(0)
        o_ref[rows, :] = jnp.where(first, outs[0], outs[1]).astype(jnp.bfloat16)
        lse_ref[rows, :] = jnp.where(first, lses[0], lses[1])


def attend_call(projected):
    _, rows, width = projected.shape
    pairs = width // 128
    spec = [pl.BlockSpec((1, rows, 128), functools.partial(lambda t, i: (t, 0, i), t)) for t in range(3)]
    return pl.pallas_call(
        attend_kernel,
        grid=(pairs,),
        out_shape=(jax.ShapeDtypeStruct((rows, width), jnp.bfloat16),
                   jax.ShapeDtypeStruct((rows, width), jnp.float32)),
        in_specs=spec,
        out_specs=(pl.BlockSpec((rows, 128), lambda i: (0, i)), pl.BlockSpec((rows, 128), lambda i: (0, i))),
        compiler_params=pltpu.CompilerParams(vmem_limit_bytes=48 * 2**20),
        cost_estimate=pl.CostEstimate(flops=4 * 10**9, bytes_accessed=6 * 10**6, transcendentals=4 * 10**6),
        name="attend",
    )(projected, projected, projected)


def attend_back_rows(block, q_ref, k_ref, v_ref, g_ref, lse_ref, dq_ref, dk_ref, dv_ref):
    scale = HD ** (-0.5)
    mask = own_mask()
    low = jnp.bfloat16
    far, start = key_ranges(block)
    rows = slice(start, start + BLOCK)
    dq = None
    for which in range(2):
        lanes = head_lanes(which)
        q = jnp.where(lanes, q_ref[rows, :], 0)
        g = jnp.where(lanes, g_ref[rows, :], 0)
        lse = lse_ref[rows, which * HD : which * HD + 1]
        k_own = jnp.where(lanes, k_ref[rows, :], 0)
        p_own = jnp.where(mask, jnp.exp(dot(q, k_own, 1, 1) * scale - lse), 0.0)
        d_own = dot(g, v_ref[rows, :], 1, 1)
        row_dot = jnp.sum(p_own * d_own, axis=-1, keepdims=True)
        if far:
            k_far = jnp.where(lanes, k_ref[0:far, :], 0)
            p_far = jnp.exp(dot(q, k_far, 1, 1) * scale - lse)
            d_far = dot(g, v_ref[0:far, :], 1, 1)
            row_dot = row_dot + jnp.sum(p_far * d_far, axis=-1, keepdims=True)
        s_own = (p_own * (d_own - row_dot)).astype(low)
        part = dot(s_own, k_own, 1, 0)
        dk_ref[rows, :] += dot(s_own, q, 0, 0)
        dv_ref[rows, :] += dot(p_own.astype(low), g, 0, 0)
        if far:
            s_far = (p_far * (d_far - row_dot)).astype(low)
            part = part + dot(s_far, k_far, 1, 0)
            dk_ref[0:far, :] += dot(s_far, q, 0, 0)
            dv_ref[0:far, :] += dot(p_far.astype(low), g, 0, 0)
        dq = part if dq is None else dq + part
    dq_ref[rows, :] = dq


PAIR_ROWS = 3072


def attend_back_kernel(q_ref, k_ref, v_ref, lse_ref, mixed_ref, cot_ref, ln1_ref, outw_ref, qkvw_ref,
                       part_ref, dn_ref, bias_ref, obias_ref, g_ref, dq_ref, dk_ref, dv_ref, d_ref):
    low, f32 = jnp.bfloat16, jnp.float32
    scale = HD ** (-0.5)
    pair = pl.program_id(0)
    g_ref[...] = dot(cot_ref[...], outw_ref[...], 1, 1).astype(low)
    grad_out = dot(mixed_ref[...], cot_ref[...], 0, 0).astype(low)
    for j in range(6):
        part_ref[j * 128 : (j + 1) * 128, :] = grad_out[:, j * 128 : (j + 1) * 128]
    dk_ref[...] = jnp.zeros_like(dk_ref)
    dv_ref[...] = jnp.zeros_like(dv_ref)
    for block in range(GROUP // BLOCK):
        attend_back_rows(block, q_ref.at[0], k_ref.at[0], v_ref.at[0], g_ref, lse_ref, dq_ref, dk_ref, dv_ref)

    @pl.when(pair == 0)
    def _():
        dn_ref[...] = jnp.zeros_like(dn_ref)
        obias_ref[...] = jnp.sum(cot_ref[...].astype(f32), axis=0, keepdims=True)

    d_ref[0] = (dq_ref[...] * scale).astype(low)
    d_ref[1] = (dk_ref[...] * scale).astype(low)
    d_ref[2] = dv_ref[...].astype(low)
    for t in range(3):
        d = d_ref[t]
        part_ref[(t + 1) * 768 : (t + 2) * 768, :] = dot(ln1_ref[...], d, 0, 0).astype(low)
        dn_ref[...] += dot(d, qkvw_ref[t], 1, 1)
        bias_ref[t : t + 1, :] = jnp.sum(d.astype(f32), axis=0, keepdims=True)


def attend_back_call(projected, lse, mixed, cot, ln1_full, out_weight, qkv_weight):
    _, rows, width = projected.shape
    pairs = width // 128
    depth = cot.shape[1]
    spec = [pl.BlockSpec((1, rows, 128), functools.partial(lambda t, i: (t, 0, i), t)) for t in range(3)]
    column = pl.BlockSpec((rows, 128), lambda i: (0, i))
    whole = pl.BlockSpec((rows, depth), lambda i: (0, 0))
    f32, low = jnp.float32, jnp.bfloat16
    return pl.pallas_call(
        attend_back_kernel,
        grid=(pairs,),
        out_shape=(jax.ShapeDtypeStruct((pairs * PAIR_ROWS, 128), low),
                   jax.ShapeDtypeStruct((rows, depth), f32),
                   jax.ShapeDtypeStruct((3, width), f32),
                   jax.ShapeDtypeStruct((1, depth), f32)),
        in_specs=spec + [column, column, whole, whole,
                         pl.BlockSpec((128, depth), lambda i: (i, 0)),
                         pl.BlockSpec((3, depth, 128), lambda i: (0, 0, i))],
        out_specs=(pl.BlockSpec((PAIR_ROWS, 128), lambda i: (i, 0)), whole,
                   pl.BlockSpec((3, 128), lambda i: (0, i)), pl.BlockSpec((1, depth), lambda i: (0, 0))),
        scratch_shapes=[pltpu.VMEM((rows, 128), low)] + [pltpu.VMEM((rows, 128), f32)] * 3
        + [pltpu.VMEM((3, rows, 128), low)],
        compiler_params=pltpu.CompilerParams(vmem_limit_bytes=56 * 2**20),
        cost_estimate=pl.CostEstimate(flops=12 * 10**9, bytes_accessed=20 * 10**6, transcendentals=4 * 10**6),
        name="attend_back",
    )(projected, projected, projected, lse, mixed, cot, ln1_full, out_weight, qkv_weight)


UNITS = 256


def mlp_kernel(x_ref, g_ref, fcw_ref, fcb_ref, pw_ref, out_ref, dn_ref, pp_ref, fp_ref, fb_ref, pb_ref):
    low, f32 = jnp.bfloat16, jnp.float32
    tile = pl.program_id(0)
    pre = dot(x_ref[...], fcw_ref[...], 1, 0) + fcb_ref[...].astype(f32)
    grad = dot(g_ref[...], pw_ref[...], 1, 1)
    coef = 0.7978845608028654
    square = pre * pre
    curve = jnp.tanh(coef * (pre + 0.044715 * (square * pre)))
    half = 0.5 * (1.0 + curve)
    act = (pre * half).astype(low)
    slope = half + 0.5 * pre * (1.0 - curve * curve) * (coef * (1.0 + 3 * 0.044715 * square))
    d_pre = (grad * slope).astype(low)

    @pl.when(tile == 0)
    def _():
        out_ref[...] = jnp.zeros_like(out_ref)
        dn_ref[...] = jnp.zeros_like(dn_ref)
        pb_ref[...] = jnp.sum(g_ref[...].astype(f32), axis=0, keepdims=True)

    fb_ref[...] = jnp.sum(d_pre.astype(f32), axis=0, keepdims=True)
    grad_proj = dot(act, g_ref[...], 0, 0).astype(low)
    for j in range(6):
        pp_ref[j * UNITS : (j + 1) * UNITS, :] = grad_proj[:, j * 128 : (j + 1) * 128]
    grad_fc = dot(x_ref[...], d_pre, 0, 0).astype(low)
    for j in range(2):
        fp_ref[j * 768 : (j + 1) * 768, :] = grad_fc[:, j * 128 : (j + 1) * 128]
    out_ref[...] += dot(act, pw_ref[...], 1, 0)
    dn_ref[...] += dot(d_pre, fcw_ref[...], 1, 1)


def mlp_call(x, g, fc_weight, fc_bias, proj_weight):
    rows, depth = x.shape
    units = fc_weight.shape[1]
    tiles = units // UNITS
    f32, low = jnp.float32, jnp.bfloat16
    whole = pl.BlockSpec((rows, depth), lambda i: (0, 0))
    item = pl.BlockSpec((ITEM, 128), lambda i: (i, 0))
    return pl.pallas_call(
        mlp_kernel,
        grid=(tiles,),
        out_shape=(jax.ShapeDtypeStruct((rows, depth), f32), jax.ShapeDtypeStruct((rows, depth), f32),
                   jax.ShapeDtypeStruct((tiles * ITEM, 128), low), jax.ShapeDtypeStruct((tiles * ITEM, 128), low),
                   jax.ShapeDtypeStruct((1, units), f32), jax.ShapeDtypeStruct((1, depth), f32)),
        in_specs=[whole, whole, pl.BlockSpec((depth, UNITS), lambda i: (0, i)),
                  pl.BlockSpec((1, UNITS), lambda i: (0, i)), pl.BlockSpec((UNITS, depth), lambda i: (i, 0))],
        out_specs=(whole, whole, item, item, pl.BlockSpec((1, UNITS), lambda i: (0, i)),
                   pl.BlockSpec((1, depth), lambda i: (0, 0))),
        compiler_params=pltpu.CompilerParams(vmem_limit_bytes=60 * 2**20),
        cost_estimate=pl.CostEstimate(flops=17 * 10**9, bytes_accessed=25 * 10**6, transcendentals=2 * 10**6),
        name="mlp",
    )(x, g, fc_weight, fc_bias.reshape(1, units), proj_weight)


def spread_kernel(p_ref, f_ref, proj_ref, fc_ref):
    f32 = jnp.float32
    for j in range(6):
        proj_ref[:, j * 128 : (j + 1) * 128] = p_ref[j * UNITS : (j + 1) * UNITS, :].astype(f32)
    for j in range(2):
        fc_ref[:, j * 128 : (j + 1) * 128] = f_ref[j * 768 : (j + 1) * 768, :].astype(f32)


def spread_call(total, units, depth):
    tiles = units // UNITS
    f32 = jnp.float32
    return pl.pallas_call(
        spread_kernel,
        grid=(tiles,),
        out_shape=(jax.ShapeDtypeStruct((units, depth), f32), jax.ShapeDtypeStruct((depth, units), f32)),
        in_specs=[pl.BlockSpec((ITEM, 128), lambda i: (i, 0)),
                  pl.BlockSpec((ITEM, 128), lambda i: (i + tiles, 0))],
        out_specs=(pl.BlockSpec((UNITS, depth), lambda i: (i, 0)), pl.BlockSpec((depth, UNITS), lambda i: (0, i))),
        compiler_params=pltpu.CompilerParams(vmem_limit_bytes=24 * 2**20),
        name="spread_mlp",
    )(total, total)


def spread_pair_kernel(a_ref, out_ref, qkv_ref):
    f32 = jnp.float32
    for j in range(6):
        out_ref[:, j * 128 : (j + 1) * 128] = a_ref[j * 128 : (j + 1) * 128, :].astype(f32)
    for t in range(3):
        qkv_ref[t] = a_ref[(t + 1) * 768 : (t + 2) * 768, :].astype(f32)


def spread_pair_call(total, first, width, depth):
    pairs = width // 128
    f32 = jnp.float32
    skip = first // PAIR_ROWS
    return pl.pallas_call(
        spread_pair_kernel,
        grid=(pairs,),
        out_shape=(jax.ShapeDtypeStruct((width, depth), f32), jax.ShapeDtypeStruct((3, depth, width), f32)),
        in_specs=[pl.BlockSpec((PAIR_ROWS, 128), lambda i: (i + skip, 0))],
        out_specs=(pl.BlockSpec((128, depth), lambda i: (i, 0)), pl.BlockSpec((3, depth, 128), lambda i: (0, 0, i))),
        compiler_params=pltpu.CompilerParams(vmem_limit_bytes=24 * 2**20),
        name="spread_attend",
    )(total)


def over_slice(values):
    count = lax.axis_size("dp")
    total = values
    for shift in range(16, count, 16):
        total = total + lax.ppermute(values, "dp", [(i, (i + shift) % count) for i in range(count)])
    return total


def on_device(
    tokens,
    ln1_gain,
    ln1_bias,
    qkv_weight,
    qv_bias,
    out_weight,
    out_bias,
    ln2_gain,
    ln2_bias,
    fc_weight,
    fc_bias,
    proj_weight,
    proj_bias,
    cotangent,
):
    own_rows = tokens.shape[0]
    group_rows = own_rows * lax.axis_size("tensor")
    local_width = qkv_weight.shape[2]
    heads_local = local_width // HD
    gain_one = ln1_gain.astype(jnp.float32)
    gain_two = ln2_gain.astype(jnp.float32)
    x_own = tokens.astype(jnp.float32)
    normed1, normal1, inv_std1 = norm_rows(x_own, gain_one, ln1_bias.astype(jnp.float32))
    ln1_full = gather_pair(normed1.astype(jnp.bfloat16))
    projected = jnp.einsum("gd,tdj->tgj", ln1_full, qkv_weight, preferred_element_type=jnp.float32)
    bias_float = qv_bias.astype(jnp.float32)
    bias_rows = jnp.stack([bias_float[0], jnp.zeros_like(bias_float[0]), bias_float[1]])
    projected = (projected + bias_rows[:, None]).astype(jnp.bfloat16)
    mixed_low, lse = attend_call(projected)
    part_rows = mixed_low
    attn_own = scatter_pair(jnp.dot(part_rows, out_weight, preferred_element_type=jnp.float32)) + out_bias.astype(jnp.float32)
    residual = x_own + attn_own
    normed2, normal2, inv_std2 = norm_rows(residual, gain_two, ln2_bias.astype(jnp.float32))
    ln2_full = gather_pair(normed2.astype(jnp.bfloat16))
    cot_full = gather_pair(cotangent)
    mlp_part, norm2_part, part_proj, part_fc, grad_fc_bias, grad_proj_bias = mlp_call(
        ln2_full, cot_full, fc_weight, fc_bias, proj_weight
    )
    block_output = (residual + (scatter_pair(mlp_part) + proj_bias.astype(jnp.float32))).astype(jnp.bfloat16)
    grad_norm2 = scatter_pair(norm2_part)
    grad_resid = cotangent.astype(jnp.float32) + norm_back(grad_norm2, normal2, inv_std2, gain_two)
    part_ln2_gain = jnp.sum(grad_norm2 * normal2, axis=0)
    part_ln2_bias = jnp.sum(grad_norm2, axis=0)
    attn_cot_full = gather_pair(grad_resid.astype(jnp.bfloat16))
    part_attn, norm1_part, grad_bias_rows, grad_out_bias = attend_back_call(
        projected, lse, mixed_low, attn_cot_full, ln1_full, out_weight, qkv_weight
    )
    grad_norm1 = scatter_pair(norm1_part)
    input_grad = (grad_resid + norm_back(grad_norm1, normal1, inv_std1, gain_one)).astype(
        jnp.bfloat16
    )
    part_ln1_gain = jnp.sum(grad_norm1 * normal1, axis=0)
    part_ln1_bias = jnp.sum(grad_norm1, axis=0)
    width = tokens.shape[1]
    units = fc_weight.shape[1]
    small = jnp.concatenate(
        [
            part_ln1_gain,
            part_ln1_bias,
            part_ln2_gain,
            part_ln2_bias,
            grad_bias_rows[0],
            grad_bias_rows[2],
            grad_out_bias[0],
            grad_fc_bias[0],
            grad_proj_bias[0],
            jnp.zeros((SMALL * 128 - 6912,), jnp.float32),
        ]
    ).reshape(SMALL, 128)
    total, small = sum_call((part_proj, part_fc, part_attn), small)
    grad_proj_weight, grad_fc_weight = spread_call(total, units, width)
    grad_out_weight, grad_qkv_weight = spread_pair_call(
        total, 2 * units * width // 128, local_width, width
    )
    small = over_slice(small)
    if lax.axis_size("dp") > 16:
        grad_proj_weight = over_slice(grad_proj_weight)
        grad_fc_weight = over_slice(grad_fc_weight)
        grad_out_weight = over_slice(grad_out_weight)
        grad_qkv_weight = over_slice(grad_qkv_weight)
    flat = small.reshape(-1)
    grad_ln1_gain, grad_ln1_bias = flat[:768], flat[768:1536]
    grad_ln2_gain, grad_ln2_bias = flat[1536:2304], flat[2304:3072]
    grad_qv_bias = flat[3072:3840].reshape(2, local_width)
    grad_out_bias, grad_fc_bias, grad_proj_bias = flat[3840:4608], flat[4608:6144], flat[6144:6912]
    return (
        block_output,
        input_grad,
        grad_ln1_gain,
        grad_ln1_bias,
        grad_qkv_weight,
        grad_qv_bias,
        grad_out_weight,
        grad_out_bias,
        grad_ln2_gain,
        grad_ln2_bias,
        grad_fc_weight,
        grad_fc_bias,
        grad_proj_weight,
        grad_proj_bias,
    )


def solution(mesh):
    return jax.shard_map(
        on_device,
        mesh=mesh,
        in_specs=(
            P(("dp", "tensor"), None),
            P(),
            P(),
            P(None, None, "tensor"),
            P(None, "tensor"),
            P("tensor", None),
            P(),
            P(),
            P(),
            P(None, "tensor"),
            P("tensor"),
            P("tensor", None),
            P(),
            P(("dp", "tensor"), None),
        ),
        out_specs=(
            P(("dp", "tensor"), None),
            P(("dp", "tensor"), None),
            P(),
            P(),
            P(None, None, "tensor"),
            P(None, "tensor"),
            P("tensor", None),
            P(),
            P(),
            P(),
            P(None, "tensor"),
            P("tensor"),
            P("tensor", None),
            P(),
        ),
        check_vma=False,
    )
```

```python
import functools
import jax
import jax.numpy as jnp
from jax import lax
from jax.experimental import pallas as pl
from jax.experimental.pallas import tpu as pltpu

from jax.sharding import PartitionSpec as P

HD = 64
PROMPT = 896
CONT = 128
NCONT = 2


EPSILON = 1e-05
MASKED = -1e30


def norm_rows(values, gain_vec, shift_vec):
    mean_row = jnp.mean(values, axis=-1, keepdims=True)
    centred = values - mean_row
    inv_std = lax.rsqrt(jnp.mean(centred * centred, axis=-1, keepdims=True) + EPSILON)
    normal = centred * inv_std
    return (normal * gain_vec + shift_vec, normal, inv_std)


def norm_back(grad_out, normal, inv_std, gain_vec):
    scaled = grad_out * gain_vec
    inner = (
        scaled
        - jnp.mean(scaled, axis=-1, keepdims=True)
        - normal * jnp.mean(scaled * normal, axis=-1, keepdims=True)
    )
    return inner * inv_std


MESH = pl.DeviceIdType.MESH
ITEM = 1536
SMALL = 56
LN_ROWS = 24


class Sum:
    def __init__(self, part, res, rx1, rx2, rx3, ssem, rsem, loc):
        self.part, self.res, self.rx1, self.rx2, self.rx3 = part, res, rx1, rx2, rx3
        self.ssem, self.rsem, self.loc = ssem, rsem, loc
        dp, t = lax.axis_index("dp"), lax.axis_index("tensor")
        x, y, z = lax.rem(dp, 2), lax.rem(lax.div(dp, 2), 2), lax.rem(lax.div(dp, 4), 4)
        self.t, self.z = t, z
        self.a = x * (1 - t) + y * t
        self.b = y * (1 - t) + x * t
        self.to_a = (dp + (1 + t) * (1 - 2 * self.a), t)
        self.to_b = (dp + (2 - t) * (1 - 2 * self.b), t)
        self.to_z = []
        self.zs = []
        for d in (1, 2, 3):
            zj = lax.rem(z + d, 4)
            self.zs.append(zj)
            self.to_z.append((dp + 4 * (zj - z), t))
        self.to_x = (dp + 1 - 2 * x, t)
        self.to_y = (dp + 2 - 4 * y, t)
        self.to_c = (dp, 1 - t)

    def barrier(self):
        bar = pltpu.get_barrier_semaphore()
        peers = [self.to_x, self.to_y, self.to_c] + self.to_z
        for peer in peers:
            pl.semaphore_signal(bar, inc=1, device_id=peer, device_id_type=MESH)
        pl.semaphore_wait(bar, len(peers))

    def rows(self, offset, count):
        return pl.ds(pl.multiple_of(offset, 32), count)

    def copy(self, src, dst, k, i, peer):
        return pltpu.make_async_remote_copy(
            src_ref=src, dst_ref=dst, send_sem=self.ssem.at[k, i], recv_sem=self.rsem.at[k, i],
            device_id=peer, device_id_type=MESH)

    def copies(self, stage, i):
        base = i * ITEM
        half = base + self.a * (ITEM // 2)
        quarter = half + self.b * (ITEM // 4)
        block = quarter + self.z * (ITEM // 16)
        if stage == 1:
            src = self.part.at[self.rows(base + (1 - self.a) * (ITEM // 2), ITEM // 2)]
            return [self.copy(src, self.rx1.at[self.rows(i * (ITEM // 2), ITEM // 2)], 0, i, self.to_a)]
        if stage == 2:
            src = self.part.at[self.rows(half + (1 - self.b) * (ITEM // 4), ITEM // 4)]
            return [self.copy(src, self.rx2.at[self.rows(i * (ITEM // 4), ITEM // 4)], 1, i, self.to_b)]
        if stage == 3:
            out = []
            for d in range(3):
                src = self.part.at[self.rows(quarter + self.zs[d] * (ITEM // 16), ITEM // 16)]
                dst = self.rx3.at[self.rows((i * 3 + d) * (ITEM // 16), ITEM // 16)]
                out.append(self.copy(src, dst, 2 + d, i, self.to_z[d]))
            return out
        if stage == 4:
            own = self.rows(block, ITEM // 16)
            return [self.copy(self.part.at[own], self.res.at[own], 5 + d, i, self.to_z[d]) for d in range(3)]
        if stage == 5:
            ref = self.res.at[self.rows(quarter, ITEM // 4)]
            return [self.copy(ref, ref, 8, i, self.to_b)]
        ref = self.res.at[self.rows(half, ITEM // 2)]
        return [self.copy(ref, ref, 9, i, self.to_a)]

    def keep(self, i):
        own = self.rows(
            i * ITEM + self.a * (ITEM // 2) + self.b * (ITEM // 4) + self.z * (ITEM // 16), ITEM // 16)
        return pltpu.make_async_copy(self.part.at[own], self.res.at[own], self.loc.at[i])

    def start(self, stage, i):
        for c in self.copies(stage, i):
            c.start()

    def arrive(self, stage, i):
        for c in self.copies(stage, i):
            c.wait_recv()
        half = i * ITEM + self.a * (ITEM // 2)
        quarter = half + self.b * (ITEM // 4)
        block = quarter + self.z * (ITEM // 16)
        f32 = jnp.float32
        if stage == 1:
            own = self.rows(half, ITEM // 2)
            got = self.rx1[self.rows(i * (ITEM // 2), ITEM // 2), :]
            self.part[own, :] = (self.part[own, :].astype(f32) + got.astype(f32)).astype(jnp.bfloat16)
        elif stage == 2:
            own = self.rows(quarter, ITEM // 4)
            got = self.rx2[self.rows(i * (ITEM // 4), ITEM // 4), :]
            self.part[own, :] = (self.part[own, :].astype(f32) + got.astype(f32)).astype(jnp.bfloat16)
        elif stage == 3:
            own = self.rows(block, ITEM // 16)
            total = self.part[own, :].astype(f32)
            for d in range(3):
                total = total + self.rx3[self.rows((i * 3 + d) * (ITEM // 16), ITEM // 16), :].astype(f32)
            self.part[own, :] = total.astype(jnp.bfloat16)
            self.keep(i).start()
        elif stage == 4:
            self.keep(i).wait()
        if stage < 6:
            self.start(stage + 1, i)

    def sent(self, i):
        for stage in range(1, 7):
            for c in self.copies(stage, i):
                c.wait_send()


def small_sum(comm, small, out, land_c, land_x, land_y, land_z, acc, ssem, rsem):
    def copy(src, dst, k, peer):
        return pltpu.make_async_remote_copy(
            src_ref=src, dst_ref=dst, send_sem=ssem.at[k], recv_sem=rsem.at[k],
            device_id=peer, device_id_type=MESH)

    c = copy(small.at[pl.ds(0, LN_ROWS)], land_c, 0, comm.to_c)
    c.start()
    yield
    c.wait_recv()
    acc[0] = small[...]
    acc[0, pl.ds(0, LN_ROWS), :] = small[pl.ds(0, LN_ROWS), :] + land_c[...]
    cx = copy(acc.at[0], land_x, 1, comm.to_x)
    cx.start()
    yield
    cx.wait_recv()
    acc[1] = acc[0] + land_x[...]
    cy = copy(acc.at[1], land_y, 2, comm.to_y)
    cy.start()
    yield
    cy.wait_recv()
    acc[2] = acc[1] + land_y[...]
    cz = []
    for d in range(3):
        cz.append(copy(acc.at[2], land_z.at[comm.z], 3 + d, comm.to_z[d]))
        cz[-1].start()
    yield
    land_z[comm.z] = acc[2]
    for d in range(3):
        cz[d].wait_recv()
    out[...] = (land_z[0] + land_z[1]) + (land_z[2] + land_z[3])
    for s in [c, cx, cy] + cz:
        s.wait_send()
    yield


def swap(values):
    return lax.ppermute(values, "tensor", [(0, 1), (1, 0)])


def gather_pair(own):
    rows = own.shape[0]
    t = lax.axis_index("tensor")
    full = jnp.zeros((2 * rows,) + own.shape[1:], own.dtype)
    full = lax.dynamic_update_slice_in_dim(full, own, t * rows, 0)
    return lax.dynamic_update_slice_in_dim(full, swap(own), (1 - t) * rows, 0)


def scatter_pair(part):
    rows = part.shape[0] // 2
    t = lax.axis_index("tensor")
    away = lax.dynamic_slice_in_dim(part, (1 - t) * rows, rows, 0)
    return lax.dynamic_slice_in_dim(part, t * rows, rows, 0) + swap(away)


def dot(lhs, rhs, lhs_dim, rhs_dim):
    return lax.dot_general(
        lhs, rhs, (((lhs_dim,), (rhs_dim,)), ((), ())), preferred_element_type=jnp.float32)


BLOCK = 128
PROMPT_BLOCKS = PROMPT // BLOCK
GROUP = PROMPT + NCONT * CONT


def head_lanes(which):
    lane = lax.broadcasted_iota(jnp.int32, (1, 128), 1)
    return (lane >= which * HD) & (lane < (which + 1) * HD)


def own_mask():
    row_pos = lax.broadcasted_iota(jnp.int32, (BLOCK, BLOCK), 0)
    col_pos = lax.broadcasted_iota(jnp.int32, (BLOCK, BLOCK), 1)
    return col_pos <= row_pos


def key_ranges(block):
    start = block * BLOCK
    return min(start, PROMPT), start


def attend_kernel(q_ref, k_ref, v_ref, o_ref, lse_ref):
    scale = HD ** (-0.5)
    mask = own_mask()
    for block in range(GROUP // BLOCK):
        far, start = key_ranges(block)
        rows = slice(start, start + BLOCK)
        outs, lses = [], []
        for which in range(2):
            lanes = head_lanes(which)
            q = jnp.where(lanes, q_ref[0, rows, :], 0)
            near = jnp.where(mask, dot(q, k_ref[0, rows, :], 1, 1) * scale, MASKED)
            top = jnp.max(near, axis=-1, keepdims=True)
            if far:
                away = dot(q, k_ref[0, 0:far, :], 1, 1) * scale
                top = jnp.maximum(top, jnp.max(away, axis=-1, keepdims=True))
            near = jnp.exp(near - top)
            total = jnp.sum(near, axis=-1, keepdims=True)
            if far:
                away = jnp.exp(away - top)
                total = total + jnp.sum(away, axis=-1, keepdims=True)
            share = 1.0 / total
            out = dot((near * share).astype(jnp.bfloat16), v_ref[0, rows, :], 1, 0)
            if far:
                out = out + dot((away * share).astype(jnp.bfloat16), v_ref[0, 0:far, :], 1, 0)
            outs.append(out)
            lses.append(top + jnp.log(total))
        first = head_lanes(0)
        o_ref[rows, :] = jnp.where(first, outs[0], outs[1]).astype(jnp.bfloat16)
        lse_ref[rows, :] = jnp.where(first, lses[0], lses[1])


def attend_call(projected):
    _, rows, width = projected.shape
    pairs = width // 128
    spec = [pl.BlockSpec((1, rows, 128), functools.partial(lambda t, i: (t, 0, i), t)) for t in range(3)]
    return pl.pallas_call(
        attend_kernel,
        grid=(pairs,),
        out_shape=(jax.ShapeDtypeStruct((rows, width), jnp.bfloat16),
                   jax.ShapeDtypeStruct((rows, width), jnp.float32)),
        in_specs=spec,
        out_specs=(pl.BlockSpec((rows, 128), lambda i: (0, i)), pl.BlockSpec((rows, 128), lambda i: (0, i))),
        compiler_params=pltpu.CompilerParams(vmem_limit_bytes=48 * 2**20),
        cost_estimate=pl.CostEstimate(flops=4 * 10**9, bytes_accessed=6 * 10**6, transcendentals=4 * 10**6),
        name="attend",
    )(projected, projected, projected)


def attend_back_rows(block, q_ref, k_ref, v_ref, g_ref, lse_ref, dq_ref, dk_ref, dv_ref):
    scale = HD ** (-0.5)
    mask = own_mask()
    low = jnp.bfloat16
    far, start = key_ranges(block)
    rows = slice(start, start + BLOCK)
    dq = None
    for which in range(2):
        lanes = head_lanes(which)
        q = jnp.where(lanes, q_ref[rows, :], 0)
        g = jnp.where(lanes, g_ref[rows, :], 0)
        lse = lse_ref[rows, which * HD : which * HD + 1]
        k_own = jnp.where(lanes, k_ref[rows, :], 0)
        p_own = jnp.where(mask, jnp.exp(dot(q, k_own, 1, 1) * scale - lse), 0.0)
        d_own = dot(g, v_ref[rows, :], 1, 1)
        row_dot = jnp.sum(p_own * d_own, axis=-1, keepdims=True)
        if far:
            k_far = jnp.where(lanes, k_ref[0:far, :], 0)
            p_far = jnp.exp(dot(q, k_far, 1, 1) * scale - lse)
            d_far = dot(g, v_ref[0:far, :], 1, 1)
            row_dot = row_dot + jnp.sum(p_far * d_far, axis=-1, keepdims=True)
        s_own = (p_own * (d_own - row_dot)).astype(low)
        part = dot(s_own, k_own, 1, 0)
        dk_ref[rows, :] += dot(s_own, q, 0, 0)
        dv_ref[rows, :] += dot(p_own.astype(low), g, 0, 0)
        if far:
            s_far = (p_far * (d_far - row_dot)).astype(low)
            part = part + dot(s_far, k_far, 1, 0)
            dk_ref[0:far, :] += dot(s_far, q, 0, 0)
            dv_ref[0:far, :] += dot(p_far.astype(low), g, 0, 0)
        dq = part if dq is None else dq + part
    dq_ref[rows, :] = dq


PAIR_ROWS = 3072


UNITS = 256


LAG = 3


def column_sum(values):
    return jnp.sum(values, axis=0, keepdims=True)


def put_vector(small, row, vector):
    for j in range(vector.shape[1] // 128):
        small[row + j : row + j + 1, :] = vector[:, j * 128 : (j + 1) * 128]


def slope_and_act(pre):
    coef = 0.7978845608028654
    square = pre * pre
    curve = jnp.tanh(coef * (pre + 0.044715 * (square * pre)))
    half = 0.5 * (1.0 + curve)
    slope = half + 0.5 * pre * (1.0 - curve * curve) * (coef * (1.0 + 3 * 0.044715 * square))
    return slope, pre * half


def back_kernel(n, tiles, pairs, *refs):
    (x_ref, g_ref, fcw_in, fcb_ref, pw_in, pb_ref, gain1, gain2, outw_in, qkvw_in, qkv_in, lse_in, mixed_in, ln1_in,
     resid_in, tok_in,
     res, small_out, block_out, input_out,
     fcw_ref, pw_ref, outw_ref, qkvw_ref, qkv_ref, lse_ref, mixed_ref, ln1_ref, resid_ref, tok_ref, lsem,
     act_ref, dpre_ref, acc0, acc1, land0, land1, dattn, gresid, dm_ref, dq_ref, dk_ref, dv_ref, d_ref,
     part, rx1, rx2, rx3, ssem, rsem, loc, psem_s, psem_r,
     small, land_c, land_x, land_y, land_z, sacc, ss, sr) = refs
    low, f32 = jnp.bfloat16, jnp.float32
    scale = HD ** (-0.5)
    comm = Sum(part, res, rx1, rx2, rx3, ssem, rsem, loc)
    loads = [
        pltpu.make_async_copy(src, dst, lsem.at[k])
        for k, (src, dst) in enumerate((
            (fcw_in, fcw_ref), (pw_in, pw_ref), (resid_in, resid_ref), (outw_in, outw_ref), (mixed_in, mixed_ref),
            (qkv_in, qkv_ref), (lse_in, lse_ref), (ln1_in, ln1_ref), (qkvw_in, qkvw_ref), (tok_in, tok_ref)))
    ]
    for load in loads:
        load.start()
    comm.barrier()
    rows, depth = x_ref.shape
    own_rows = rows // 2
    own = pl.ds(pl.multiple_of(comm.t * own_rows, 64), own_rows)
    away = pl.ds(pl.multiple_of((1 - comm.t) * own_rows, 64), own_rows)

    def pair_copy(src, dst, k):
        return pltpu.make_async_remote_copy(
            src_ref=src, dst_ref=dst, send_sem=psem_s.at[k], recv_sem=psem_r.at[k],
            device_id=comm.to_c, device_id_type=MESH)

    def wave(w):
        for stage in range(1, 7):
            i = w - (stage - 1)

            @pl.when((i >= 0) & (i < n))
            def _():
                comm.arrive(stage, i)

    small[...] = jnp.zeros_like(small)
    put_vector(small, 48, column_sum(g_ref[...].astype(f32)))
    acc0[...] = jnp.zeros_like(acc0)
    acc1[...] = jnp.zeros_like(acc1)
    loads[0].wait()
    loads[1].wait()

    def tile_step(k, carry):
        units = pl.ds(pl.multiple_of(k * UNITS, UNITS), UNITS)
        bias = fcb_ref[0:1, units].astype(f32)
        for part_rows in range(2):
            chunk = slice(part_rows * own_rows, (part_rows + 1) * own_rows)
            pre = dot(x_ref[chunk, :], fcw_ref[:, units], 1, 0) + bias
            slope, act = slope_and_act(pre)
            act_ref[chunk, :] = act.astype(low)
            dpre_ref[chunk, :] = (dot(g_ref[chunk, :], pw_ref[units, :], 1, 1) * slope).astype(low)
        base = pl.multiple_of(k * 2 * ITEM, ITEM)
        grad_proj = dot(act_ref[...], g_ref[...], 0, 0).astype(low)
        for j in range(6):
            part[pl.ds(base + j * UNITS, UNITS), :] = grad_proj[:, j * 128 : (j + 1) * 128]
        grad_fc = dot(x_ref[...], dpre_ref[...], 0, 0).astype(low)
        for j in range(2):
            part[pl.ds(base + ITEM + j * 768, 768), :] = grad_fc[:, j * 128 : (j + 1) * 128]
        comm.start(1, 2 * k)
        comm.start(1, 2 * k + 1)
        sums = column_sum(dpre_ref[...].astype(f32))
        for j in range(2):
            small[pl.ds(36 + 2 * k + j, 1), :] = sums[:, j * 128 : (j + 1) * 128]
        for part_rows in range(2):
            chunk = slice(part_rows * own_rows, (part_rows + 1) * own_rows)
            acc1[chunk, :] += dot(dpre_ref[chunk, :], fcw_ref[:, units], 1, 1)
            acc0[chunk, :] += dot(act_ref[chunk, :], pw_ref[units, :], 1, 0)
        wave(k - LAG)
        return carry

    lax.fori_loop(0, tiles, tile_step, 0)
    send_dn = pair_copy(acc1.at[away], land1, 0)
    send_dn.start()
    send_out = pair_copy(acc0.at[away], land0, 1)
    send_out.start()
    loads[2].wait()
    gain = gain2[0:1, :].astype(f32)
    cot = g_ref[own, :].astype(f32)
    send_dn.wait_recv()
    resid = resid_ref[...]
    centred = resid - jnp.mean(resid, axis=-1, keepdims=True)
    inv_std = lax.rsqrt(jnp.mean(centred * centred, axis=-1, keepdims=True) + EPSILON)
    normal = centred * inv_std
    grad_norm = acc1[own, :] + land1[...]
    put_vector(small, 12, column_sum(grad_norm * normal))
    put_vector(small, 18, column_sum(grad_norm))
    gresid[...] = cot + norm_back(grad_norm, normal, inv_std, gain)
    dattn[own, :] = gresid[...].astype(low)
    send_cot = pair_copy(dattn.at[own], dattn.at[own], 2)
    send_cot.start()
    send_out.wait_recv()
    block_out[...] = (resid_ref[...] + (acc0[own, :] + land0[...] + pb_ref[0:1, :].astype(f32))).astype(low)
    send_out.wait_send()
    send_dn.wait_send()
    for load in loads[3:]:
        load.wait()
    acc0[...] = jnp.zeros_like(acc0)
    pair_copy(dattn.at[away], dattn.at[away], 2).wait_recv()
    put_vector(small, 30, column_sum(dattn[...].astype(f32)))

    def pair_step(p, carry):
        lanes = pl.ds(pl.multiple_of(p * 128, 128), 128)
        dm_ref[...] = dot(dattn[...], outw_ref[pl.ds(pl.multiple_of(p * 128, 128), 128), :], 1, 1).astype(low)
        base = pl.multiple_of(2 * tiles * ITEM + p * PAIR_ROWS, ITEM)
        grad_out = dot(mixed_ref[:, lanes], dattn[...], 0, 0).astype(low)
        for j in range(6):
            part[pl.ds(base + j * 128, 128), :] = grad_out[:, j * 128 : (j + 1) * 128]
        dk_ref[...] = jnp.zeros_like(dk_ref)
        dv_ref[...] = jnp.zeros_like(dv_ref)
        views = [qkv_ref.at[t, :, lanes] for t in range(3)] + [dm_ref, lse_ref.at[:, lanes]]
        for block in range(GROUP // BLOCK):
            attend_back_rows(block, *views, dq_ref, dk_ref, dv_ref)
            if block % 3 == 2:
                wave(tiles - LAG + 3 * p + block // 3)
        d_ref[0] = (dq_ref[...] * scale).astype(low)
        d_ref[1] = (dk_ref[...] * scale).astype(low)
        d_ref[2] = dv_ref[...].astype(low)
        for t in range(3):
            part[pl.ds(base + (t + 1) * 768, 768), :] = dot(ln1_ref[...], d_ref[t], 0, 0).astype(low)
        comm.start(1, 2 * tiles + 2 * p)
        comm.start(1, 2 * tiles + 2 * p + 1)
        for t in range(3):
            for part_rows in range(2):
                chunk = slice(part_rows * own_rows, (part_rows + 1) * own_rows)
                acc0[chunk, :] += dot(d_ref[t, chunk, :], qkvw_ref[t, :, lanes], 1, 1)
        small[pl.ds(24 + p, 1), :] = column_sum(d_ref[0].astype(f32))
        small[pl.ds(27 + p, 1), :] = column_sum(d_ref[2].astype(f32))
        return carry

    lax.fori_loop(0, pairs, pair_step, 0)
    send_dn = pair_copy(acc0.at[away], land1, 3)
    send_dn.start()
    tokens = tok_ref[...].astype(f32)
    centred = tokens - jnp.mean(tokens, axis=-1, keepdims=True)
    inv_std = lax.rsqrt(jnp.mean(centred * centred, axis=-1, keepdims=True) + EPSILON)
    normal = centred * inv_std
    send_dn.wait_recv()
    grad_norm = acc0[own, :] + land1[...]
    put_vector(small, 0, column_sum(grad_norm * normal))
    put_vector(small, 6, column_sum(grad_norm))
    input_out[...] = (gresid[...] + norm_back(grad_norm, normal, inv_std, gain1[0:1, :].astype(f32))).astype(low)
    send_dn.wait_send()
    send_cot.wait_send()
    sm = small_sum(comm, small, small_out, land_c, land_x, land_y, land_z, sacc, ss, sr)
    next(sm)
    first = tiles - LAG + 3 * pairs
    last = n + 5
    for mark in range(4):
        lax.fori_loop(first + mark * (last - first) // 4, first + (mark + 1) * (last - first) // 4,
                      lambda w, c: (wave(w), c)[1], 0)
        next(sm)
    lax.fori_loop(0, n, lambda i, c: (comm.sent(i), c)[1], 0)


def back_call(x, g, fc_weight, fc_bias, proj_weight, proj_bias, gain1, gain2, out_weight, qkv_weight, projected, lse,
              mixed, ln1_full, residual, tokens):
    rows, depth = x.shape
    units = fc_weight.shape[1]
    width = out_weight.shape[0]
    tiles, pairs = units // UNITS, width // 128
    n = 2 * tiles + 2 * pairs
    f32, bf = jnp.float32, jnp.bfloat16
    near, far = pl.BlockSpec(memory_space=pltpu.VMEM), pl.BlockSpec(memory_space=pl.ANY)
    late = [fc_weight, proj_weight, out_weight, qkv_weight, projected, lse, mixed, ln1_full, residual, tokens]
    own_rows = rows // 2
    dma = pltpu.SemaphoreType.DMA
    return pl.pallas_call(
        functools.partial(back_kernel, n, tiles, pairs),
        out_shape=(jax.ShapeDtypeStruct((n * ITEM, 128), bf), jax.ShapeDtypeStruct((SMALL, 128), f32),
                   jax.ShapeDtypeStruct((own_rows, depth), bf), jax.ShapeDtypeStruct((own_rows, depth), bf)),
        in_specs=[near, near, far, near, far, near, near, near] + [far] * 8,
        out_specs=(far, near, near, near),
        scratch_shapes=[pltpu.VMEM(a.shape, a.dtype) for a in late] + [dma((10,))] + [
            pltpu.VMEM((rows, UNITS), bf), pltpu.VMEM((rows, UNITS), bf),
            pltpu.VMEM((rows, depth), f32), pltpu.VMEM((rows, depth), f32),
            pltpu.VMEM((own_rows, depth), f32), pltpu.VMEM((own_rows, depth), f32),
            pltpu.VMEM((rows, depth), bf), pltpu.VMEM((own_rows, depth), f32),
            pltpu.VMEM((rows, 128), bf)] + [pltpu.VMEM((rows, 128), f32)] * 3 + [
            pltpu.VMEM((3, rows, 128), bf),
            pltpu.VMEM((n * ITEM, 128), bf),
            pltpu.VMEM((n * ITEM // 2, 128), bf),
            pltpu.VMEM((n * ITEM // 4, 128), bf),
            pltpu.VMEM((n * 3 * ITEM // 16, 128), bf),
            dma((10, n)), dma((10, n)), dma((n,)), dma((4,)), dma((4,)),
            pltpu.VMEM((SMALL, 128), f32),
            pltpu.VMEM((LN_ROWS, 128), f32),
            pltpu.VMEM((SMALL, 128), f32),
            pltpu.VMEM((SMALL, 128), f32),
            pltpu.VMEM((4, SMALL, 128), f32),
            pltpu.VMEM((3, SMALL, 128), f32),
            dma((6,)), dma((6,)),
        ],
        compiler_params=pltpu.CompilerParams(
            collective_id=0, has_side_effects=True, vmem_limit_bytes=67043328),
        cost_estimate=pl.CostEstimate(flops=30 * 10**9, bytes_accessed=40 * 10**6, transcendentals=6 * 10**6),
        name="back",
    )(x, g, fc_weight, fc_bias.reshape(1, units), proj_weight, proj_bias.reshape(1, depth),
      gain1.reshape(1, depth), gain2.reshape(1, depth), out_weight, qkv_weight, projected, lse, mixed, ln1_full,
      residual, tokens)


def spread_kernel(p_ref, f_ref, proj_ref, fc_ref):
    f32 = jnp.float32
    for j in range(6):
        proj_ref[:, j * 128 : (j + 1) * 128] = p_ref[j * UNITS : (j + 1) * UNITS, :].astype(f32)
    for j in range(2):
        fc_ref[:, j * 128 : (j + 1) * 128] = f_ref[j * 768 : (j + 1) * 768, :].astype(f32)


def spread_call(total, units, depth):
    tiles = units // UNITS
    f32 = jnp.float32
    return pl.pallas_call(
        spread_kernel,
        grid=(tiles,),
        out_shape=(jax.ShapeDtypeStruct((units, depth), f32), jax.ShapeDtypeStruct((depth, units), f32)),
        in_specs=[pl.BlockSpec((ITEM, 128), lambda i: (2 * i, 0)),
                  pl.BlockSpec((ITEM, 128), lambda i: (2 * i + 1, 0))],
        out_specs=(pl.BlockSpec((UNITS, depth), lambda i: (i, 0)), pl.BlockSpec((depth, UNITS), lambda i: (0, i))),
        compiler_params=pltpu.CompilerParams(vmem_limit_bytes=24 * 2**20),
        name="spread_mlp",
    )(total, total)


def spread_pair_kernel(a_ref, out_ref, qkv_ref):
    f32 = jnp.float32
    for j in range(6):
        out_ref[:, j * 128 : (j + 1) * 128] = a_ref[j * 128 : (j + 1) * 128, :].astype(f32)
    for t in range(3):
        qkv_ref[t] = a_ref[(t + 1) * 768 : (t + 2) * 768, :].astype(f32)


def spread_pair_call(total, first, width, depth):
    pairs = width // 128
    f32 = jnp.float32
    skip = first // PAIR_ROWS
    return pl.pallas_call(
        spread_pair_kernel,
        grid=(pairs,),
        out_shape=(jax.ShapeDtypeStruct((width, depth), f32), jax.ShapeDtypeStruct((3, depth, width), f32)),
        in_specs=[pl.BlockSpec((PAIR_ROWS, 128), lambda i: (i + skip, 0))],
        out_specs=(pl.BlockSpec((128, depth), lambda i: (i, 0)), pl.BlockSpec((3, depth, 128), lambda i: (0, 0, i))),
        compiler_params=pltpu.CompilerParams(vmem_limit_bytes=24 * 2**20),
        name="spread_attend",
    )(total)


def over_slice(values):
    count = lax.axis_size("dp")
    total = values
    for shift in range(16, count, 16):
        total = total + lax.ppermute(values, "dp", [(i, (i + shift) % count) for i in range(count)])
    return total


def on_device(
    tokens,
    ln1_gain,
    ln1_bias,
    qkv_weight,
    qv_bias,
    out_weight,
    out_bias,
    ln2_gain,
    ln2_bias,
    fc_weight,
    fc_bias,
    proj_weight,
    proj_bias,
    cotangent,
):
    own_rows = tokens.shape[0]
    group_rows = own_rows * lax.axis_size("tensor")
    local_width = qkv_weight.shape[2]
    heads_local = local_width // HD
    gain_one = ln1_gain.astype(jnp.float32)
    gain_two = ln2_gain.astype(jnp.float32)
    x_own = tokens.astype(jnp.float32)
    normed1, normal1, inv_std1 = norm_rows(x_own, gain_one, ln1_bias.astype(jnp.float32))
    ln1_full = gather_pair(normed1.astype(jnp.bfloat16))
    projected = jnp.einsum("gd,tdj->tgj", ln1_full, qkv_weight, preferred_element_type=jnp.float32)
    bias_float = qv_bias.astype(jnp.float32)
    bias_rows = jnp.stack([bias_float[0], jnp.zeros_like(bias_float[0]), bias_float[1]])
    projected = (projected + bias_rows[:, None]).astype(jnp.bfloat16)
    mixed_low, lse = attend_call(projected)
    part_rows = mixed_low
    attn_own = scatter_pair(jnp.dot(part_rows, out_weight, preferred_element_type=jnp.float32)) + out_bias.astype(jnp.float32)
    residual = x_own + attn_own
    normed2, normal2, inv_std2 = norm_rows(residual, gain_two, ln2_bias.astype(jnp.float32))
    ln2_full = gather_pair(normed2.astype(jnp.bfloat16))
    cot_full = gather_pair(cotangent)
    width = tokens.shape[1]
    units = fc_weight.shape[1]
    total, small, block_output, input_grad = back_call(
        ln2_full, cot_full, fc_weight, fc_bias, proj_weight, proj_bias, ln1_gain, ln2_gain, out_weight, qkv_weight,
        projected, lse, mixed_low, ln1_full, residual, tokens
    )
    grad_proj_weight, grad_fc_weight = spread_call(total, units, width)
    grad_out_weight, grad_qkv_weight = spread_pair_call(
        total, 2 * units * width // 128, local_width, width
    )
    small = over_slice(small)
    if lax.axis_size("dp") > 16:
        grad_proj_weight = over_slice(grad_proj_weight)
        grad_fc_weight = over_slice(grad_fc_weight)
        grad_out_weight = over_slice(grad_out_weight)
        grad_qkv_weight = over_slice(grad_qkv_weight)
    flat = small.reshape(-1)
    grad_ln1_gain, grad_ln1_bias = flat[:768], flat[768:1536]
    grad_ln2_gain, grad_ln2_bias = flat[1536:2304], flat[2304:3072]
    grad_qv_bias = flat[3072:3840].reshape(2, local_width)
    grad_out_bias, grad_fc_bias, grad_proj_bias = flat[3840:4608], flat[4608:6144], flat[6144:6912]
    return (
        block_output,
        input_grad,
        grad_ln1_gain,
        grad_ln1_bias,
        grad_qkv_weight,
        grad_qv_bias,
        grad_out_weight,
        grad_out_bias,
        grad_ln2_gain,
        grad_ln2_bias,
        grad_fc_weight,
        grad_fc_bias,
        grad_proj_weight,
        grad_proj_bias,
    )


def solution(mesh):
    return jax.shard_map(
        on_device,
        mesh=mesh,
        in_specs=(
            P(("dp", "tensor"), None),
            P(),
            P(),
            P(None, None, "tensor"),
            P(None, "tensor"),
            P("tensor", None),
            P(),
            P(),
            P(),
            P(None, "tensor"),
            P("tensor"),
            P("tensor", None),
            P(),
            P(("dp", "tensor"), None),
        ),
        out_specs=(
            P(("dp", "tensor"), None),
            P(("dp", "tensor"), None),
            P(),
            P(),
            P(None, None, "tensor"),
            P(None, "tensor"),
            P("tensor", None),
            P(),
            P(),
            P(),
            P(None, "tensor"),
            P("tensor"),
            P("tensor", None),
            P(),
        ),
        check_vma=False,
    )
```
